32 devices in a mesh: wrow: 4 (over y, core), wcol: 2 (over x), dom: 4 (over z).
Axes of the slice: x: 2, y: 2, z: 4, core: 2. Of those that a mesh axis runs over, the one named last changes fastest.
Arguments:
- positions: float32 [4, 2, 3, 8192], P('wrow', 'wcol', None, 'dom'), may hold values from -6 to 6
- velocities: float32 [4, 2, 3, 8192], P('wrow', 'wcol', None, 'dom'), may hold values from -6 to 6
- inv_mass: float32 [8192], P('dom'), may hold values from 0.5 to 2
- cv_weight: float32 [2, 3, 8192], P(None, None, 'dom'), may hold values from -0.125 to 0.125
- stiffness: float32 [2], replicated, may hold values from 1 to 4
- centers: float32 [4, 2, 2], P('wrow', 'wcol'), may hold values from -3 to 3
- block_order: int32 [8192], P('dom'), may hold values from 0 to 2047, as said below
- pair_count: int32 [4], P('dom'), may hold values from 16 to 64, as said below
- pair_own: int32 [4, 64], P('dom'), may hold values from 0 to 15, as said below
- pair_other: int32 [4, 64], P('dom'), may hold values from 0 to 47, as said below
- accept_row: int32 [4, 2], P('wrow', 'wcol'), may hold values from 0 to 1, as said below
- accept_col: int32 [4, 2], P('wrow', 'wcol'), may hold values from 0 to 1, as said below
Outputs:
- new_positions: float32 [4, 2, 3, 8192], P('wrow', 'wcol', None, 'dom')
- new_velocities: float32 [4, 2, 3, 8192], P('wrow', 'wcol', None, 'dom')
- new_forces: float32 [4, 2, 3, 8192], P('wrow', 'wcol', None, 'dom')
The draws below stay inside these ranges and needn't reach their ends.
Inputs may be any that keep to these rules, and one draw needn't show every extreme that they name: accept_row is equal for windows (2k, c) and (2k + 1, c). accept_col is equal for windows (r, 2k) and (r, 2k + 1). `block_order`: each slab's 2048 entries are a permutation of 0 to 2047. `pair_count`: some slab has exactly 64 live pairs. `pair_own`: entries past the slab's pair_count are 0. `pair_other`: slab 0 names no lower slab and the last slab no upper slab; entries past the slab's pair_count are 16.
All inputs are finite; a program needn't handle non-finite values.
Results may differ from the reference program's by a relative error of at most 0.0003.
Values sent between devices are 32-bit elements; how exact they have to be, the bound alone decides.
No kernel may reach another device: no remote copies, remote signals or barrier semaphores. Data moves between devices by JAX's collectives and lax.ppermute only.
A program may use at most 64 MiB of HBM per device.

```python
import math
import jax
import jax.numpy as jnp
from jax import lax

ATOM_DEV = 2048
BLK = 128
STEPS = 3
NB = 16
PMAX = 64
ATOMS = 8192
NROW = 4
NCOL = 2


def counts_of(key):
    domains = ATOMS // ATOM_DEV
    base = jax.random.randint(jax.random.fold_in(key, 11), (domains,), PMAX // 4, PMAX + 1)
    chosen = jax.random.randint(jax.random.fold_in(key, 12), (), 0, domains)
    return jnp.where(jnp.arange(domains) == chosen, PMAX, base).astype(jnp.int32)


def live_slots(key):
    return jnp.arange(PMAX)[None, :] < counts_of(key)[:, None]


def draw_pair_count(key, part):
    return counts_of(key)


def draw_pair_own(key, part):
    domains = ATOMS // ATOM_DEV
    raw_blocks = jax.random.randint(jax.random.fold_in(key, 13), (domains, PMAX), 0, NB)
    return jnp.where(live_slots(key), raw_blocks, 0).astype(jnp.int32)


def draw_pair_other(key, part):
    domains = ATOMS // ATOM_DEV
    raw_blocks = jax.random.randint(jax.random.fold_in(key, 14), (domains, PMAX), 0, 3 * NB)
    slab_ids = jnp.arange(domains)[:, None]
    raw_blocks = jnp.where((slab_ids == 0) & (raw_blocks < NB), raw_blocks + NB, raw_blocks)
    raw_blocks = jnp.where((slab_ids == domains - 1) & (raw_blocks >= 2 * NB), raw_blocks - NB, raw_blocks)
    return jnp.where(live_slots(key), raw_blocks, NB).astype(jnp.int32)


def draw_block_order(key, part):
    domains = ATOMS // ATOM_DEV

    def one_slab(slab):
        return jax.random.permutation(jax.random.fold_in(key, 31 + slab), ATOM_DEV)
    return jax.vmap(one_slab)(jnp.arange(domains)).reshape(ATOMS).astype(jnp.int32)


def draw_accept_row(key, part):
    halves = jax.random.randint(jax.random.fold_in(key, 21), (NROW // 2, NCOL), 0, 2)
    halves = halves.at[0, 0].set(1).at[0, 1].set(0)
    return jnp.repeat(halves, 2, axis=0).astype(jnp.int32)


def draw_accept_col(key, part):
    halves = jax.random.randint(jax.random.fold_in(key, 22), (NROW, NCOL // 2), 0, 2)
    halves = halves.at[0, 0].set(1).at[1, 0].set(0)
    return jnp.repeat(halves, 2, axis=1).astype(jnp.int32)


def steps_of(stream_key, dims, cuts, smallest, largest):
    loudness = 1.0
    for axis_at, shards_of in cuts:
        heights = jax.random.uniform(jax.random.fold_in(jax.random.fold_in(stream_key, 6), axis_at), (shards_of,), jnp.float32, smallest / len(cuts), largest / len(cuts))
        loudness = loudness * jnp.repeat(jnp.exp(heights), dims[axis_at] // shards_of).reshape((-1,) + (1,) * (len(dims) - 1 - axis_at))
    return loudness


def scatter_about(key, extent, width, most, split=(), held_as=jnp.bfloat16):
    array = width * jax.random.normal(key, extent, jnp.float32)
    if split:
        array = array * steps_of(key, extent, split, -0.22, 0.18)
    return jnp.clip(array, -most, most).astype(held_as)


def setup_inputs(seed: int = 0) -> dict:
    seeds = jax.random.split(jax.random.key(seed), 13)
    return {
        "positions": scatter_about(seeds[0], (NROW, NCOL, 3, ATOMS), 1.0, 6.0, ((0, 4), (1, 2), (3, 4)), jnp.float32),
        "velocities": scatter_about(seeds[1], (NROW, NCOL, 3, ATOMS), 1.0, 6.0, ((0, 4), (1, 2), (3, 4)), jnp.float32),
        "inv_mass": jnp.clip(jnp.exp(math.log(2.0) - 1.3862944 * jax.random.uniform(seeds[2], (ATOMS,), jnp.float32) ** steps_of(seeds[2], (ATOMS,), ((0, 4),), -0.2, 0.2)), 0.5, 2.0),
        "cv_weight": scatter_about(seeds[3], (2, 3, ATOMS), ATOM_DEV ** -0.5, 0.125, ((2, 4),), jnp.float32),
        "stiffness": jnp.clip(jnp.exp(jax.random.uniform(seeds[4], (2,), jnp.float32, math.log(1.0), math.log(4.0))), 1.0, 4.0),
        "centers": jnp.clip(jax.random.uniform(seeds[5], (NROW, NCOL, 2), jnp.float32, -3.0, 3.0) * steps_of(seeds[5], (NROW, NCOL, 2), ((0, 4), (1, 2)), -0.4, 0.0), -3.0, 3.0),
        "block_order": draw_block_order(jax.random.fold_in(seeds[12], 71), 0),
        "pair_count": draw_pair_count(jax.random.fold_in(seeds[12], 71), 0),
        "pair_own": draw_pair_own(jax.random.fold_in(seeds[12], 71), 0),
        "pair_other": draw_pair_other(jax.random.fold_in(seeds[12], 71), 0),
        "accept_row": draw_accept_row(jax.random.fold_in(seeds[12], 71), 0),
        "accept_col": draw_accept_col(jax.random.fold_in(seeds[12], 71), 0),
    }


PAIR_EPS = 0.015625
DT = 0.1


def pair_tile(own_tile, other_tile):
    offsets = own_tile[:, :, None] - other_tile[:, None, :]
    squared = jnp.sum(offsets * offsets, axis=0)
    weight_tile = PAIR_EPS * jnp.exp(-0.5 * squared)
    return own_tile * jnp.sum(weight_tile, axis=1)[None, :] - jnp.dot(other_tile, weight_tile.T, precision=lax.Precision.HIGHEST)


def domain_forces(nearby, pair_total, own_blocks, other_blocks):
    blocks_dev = ATOM_DEV // BLK

    def add_tile(forces_acc, index):
        own_index = own_blocks[index]
        other_index = other_blocks[index]
        own_tile = lax.dynamic_slice(nearby, (jnp.int32(0), ((blocks_dev + own_index) * BLK).astype(jnp.int32)), (3, BLK))
        other_tile = lax.dynamic_slice(nearby, (jnp.int32(0), (other_index * BLK).astype(jnp.int32)), (3, BLK))
        live = (index < pair_total).astype(forces_acc.dtype)
        offset = (own_index * BLK).astype(jnp.int32)
        older = lax.dynamic_slice(forces_acc, (jnp.int32(0), offset), (3, BLK))
        forces_acc = lax.dynamic_update_slice(forces_acc, older + live * pair_tile(own_tile, other_tile), (jnp.int32(0), offset))
        return forces_acc, None

    forces_acc, _ = lax.scan(add_tile, jnp.zeros((3, ATOM_DEV), jnp.float32), jnp.arange(PMAX, dtype=jnp.int32))
    return forces_acc


def window_pair(coords, pair_count, pair_own, pair_other):
    domains = ATOMS // ATOM_DEV
    slab_rows = coords.reshape(3, domains, ATOM_DEV)
    zeros_slab = jnp.zeros((3, 1, ATOM_DEV), coords.dtype)
    padded = jnp.concatenate([zeros_slab, slab_rows, zeros_slab], axis=1)
    nearby = jnp.stack([padded[:, slab:slab + 3].reshape(3, 3 * ATOM_DEV) for slab in range(domains)])
    forces_all = jax.vmap(domain_forces)(nearby, pair_count, pair_own, pair_other)
    return jnp.transpose(forces_all, (1, 0, 2)).reshape(3, ATOMS)


def total_force(coords, weights, stiffness, centre_rows, pair_count, pair_own, pair_other):
    pair = jax.vmap(window_pair, in_axes=(0, None, None, None))(coords, pair_count, pair_own, pair_other)
    collective = jnp.sum(weights[None] * coords[:, None], axis=(2, 3))
    pull = stiffness[None, :] * (collective - centre_rows)
    return pair - jnp.sum(pull[:, :, None, None] * weights[None], axis=1)


def partner_select(state, flags, axis):
    count_axis = state.shape[axis]
    swapped = jnp.take(state, jnp.arange(count_axis, dtype=jnp.int32) ^ 1, axis=axis)
    return jnp.where((flags == 1)[:, :, None, None], swapped, state)


def reference(positions, velocities, inv_mass, cv_weight, stiffness, centers, block_order, pair_count, pair_own, pair_other, accept_row, accept_col):
    domains = ATOMS // ATOM_DEV
    windows = NROW * NCOL
    global_order = (block_order.reshape(domains, ATOM_DEV) + (jnp.arange(domains, dtype=jnp.int32) * ATOM_DEV)[:, None]).reshape(ATOMS).astype(jnp.int32)
    inverse = jnp.zeros((ATOMS,), jnp.int32).at[global_order].set(jnp.arange(ATOMS, dtype=jnp.int32))
    coords = positions.reshape(windows, 3, ATOMS)[:, :, global_order]
    speeds = velocities.reshape(windows, 3, ATOMS)[:, :, global_order]
    inverse_mass = inv_mass[global_order]
    weights = cv_weight[:, :, global_order]
    centre_rows = centers.reshape(windows, 2)
    forces_now = total_force(coords, weights, stiffness, centre_rows, pair_count, pair_own, pair_other)
    for _ in range(STEPS):
        speeds = speeds + (0.5 * DT) * inverse_mass * forces_now
        coords = coords + DT * speeds
        forces_now = total_force(coords, weights, stiffness, centre_rows, pair_count, pair_own, pair_other)
        speeds = speeds + (0.5 * DT) * inverse_mass * forces_now
    results = []
    for state in (coords, speeds, forces_now):
        state = state[:, :, inverse].reshape(NROW, NCOL, 3, ATOMS)
        state = partner_select(state, accept_row, 0)
        state = partner_select(state, accept_col, 1)
        results.append(state)
    return (results[0], results[1], results[2])
```

```python
import functools
import math

import jax
import jax.numpy as jnp
from jax import lax
from jax.experimental import pallas as pl
from jax.experimental.pallas import tpu as pltpu
from jax.sharding import PartitionSpec as P

BLK = 128
STEPS = 3
PAIR_EPS = 0.015625
DT = 0.1
UNROLL = 4
ROOT = math.sqrt(math.log2(math.e))


def rounded(x):
    return x.astype(jnp.bfloat16).astype(jnp.float32)


def lanes_from(source, low):
    return jnp.take_along_axis(source, low, axis=1, mode="promise_in_bounds")


def kernel(slabs, blocks, slots, *refs):
    own_ref, other_ref, count_ref, stiff_ref = refs[:4]
    dyn_refs = refs[4 : 4 + slabs]
    stat_refs = refs[4 + slabs : 4 + 2 * slabs]
    x_out, v_out, f_out = refs[4 + 2 * slabs : 7 + 2 * slabs]
    xs, vs, ms, w0s, w1s, acc, atab, ctab, htab, inv, packed = refs[7 + 2 * slabs :]
    row = lax.broadcasted_iota(jnp.int32, (8, BLK), 0)
    fourth = (row == 3) | (row == 7)
    centre = [dyn_refs[0][3:4, k : k + 1] for k in range(2)]

    def doubled(value):
        turned = pltpu.roll(value, 4, 0)
        return jnp.where(row < 4, value, turned), jnp.where(row < 4, turned, value)

    def total4(value):
        value = value + pltpu.roll(value, 1, 0)
        return value + pltpu.roll(value, 2, 0)

    def tables(block, x):
        scaled = jnp.where(fourth, 0.0, x * ROOT)
        half = -0.5 * total4(scaled * scaled)
        base = jnp.where(fourth, half, scaled)
        s1 = rounded(base)
        rest = base - s1
        s2 = rounded(rest)
        s3 = rest - s2
        one = jnp.float32(1.0)
        zero = jnp.zeros_like(x)
        a0 = jnp.where(row == 7, s2, s1)
        a1 = jnp.where(row == 3, s3, jnp.where(row == 7, one, s2))
        a2 = jnp.where(row < 3, s1, jnp.where(fourth, one, s3))
        atab[block] = jnp.concatenate([a0, a1, a2, zero], 0).astype(jnp.bfloat16)
        c0 = jnp.where(row < 3, s1, jnp.where(fourth, one, s2))
        c1 = jnp.where((row < 3) | (row == 7), s1, jnp.where(row == 3, one, s2))
        c2 = jnp.where((row < 3) | (row == 7), s3, jnp.where(row == 3, s2, s1))
        ctab[block] = jnp.concatenate([c0, c1, c2, zero], 0).T.astype(jnp.bfloat16)
        h0 = jnp.where(row == 3, one, jnp.where(row == 7, 0.0, jnp.where(row < 4, s1, s2)))
        h1 = jnp.where(row < 3, s3, 0.0)
        htab[block] = jnp.concatenate([h0, h1], 0).astype(jnp.bfloat16)
        acc[block] = jnp.zeros((16, BLK), jnp.float32)

    def whole(value):
        return jnp.sum(jnp.sum(value, axis=0, keepdims=True), axis=1, keepdims=True)

    sums = (jnp.zeros((8, BLK), jnp.float32), jnp.zeros((8, BLK), jnp.float32))

    for slab in range(slabs):

        def bring(t, carry, slab=slab):
            dyn, stat = dyn_refs[slab], stat_refs[slab]
            first = pl.multiple_of(t * BLK, BLK)
            index = stat[7:8, pl.ds(first, BLK)].astype(jnp.int32)
            index = jnp.broadcast_to(index, (8, BLK))
            high, low = index // BLK, index % BLK
            state = jnp.zeros((8, BLK), jnp.float32)
            fixed = jnp.zeros((8, BLK), jnp.float32)
            for b in range(blocks):
                here = high == b
                state = jnp.where(here, lanes_from(dyn[:, b * BLK : (b + 1) * BLK], low), state)
                fixed = jnp.where(here, lanes_from(stat[:, b * BLK : (b + 1) * BLK], low), fixed)
            block = slab * blocks + t
            x, v = doubled(state)
            w0, w1 = doubled(jnp.where(fourth, 0.0, fixed))
            xs[block] = x
            vs[block] = v
            w0s[block] = w0
            w1s[block] = w1
            ms[block] = jnp.broadcast_to(fixed[3:4], (8, BLK))
            tables(block, x)
            return carry[0] + w0 * x, carry[1] + w1 * x

        sums = lax.fori_loop(0, blocks, bring, sums)

    def pulls(pair):
        return [
            stiff_ref[k] * (0.5 * whole(pair[k]) - centre[k]) for k in range(2)
        ]

    def tiles(slab):
        live = count_ref[slab]

        def some(group, _):
            owners, parts = [], []
            for u in range(UNROLL):
                p = group * UNROLL + u
                own = jnp.where(p < live, own_ref[slab, p] + slab * blocks, slabs * blocks)
                other = other_ref[slab, p] + (slab + slabs - 1) * blocks
                other = jnp.where(other >= slabs * blocks, other - slabs * blocks, other)
                other = jnp.where(other >= slabs * blocks, other - slabs * blocks, other)
                spread = jnp.dot(
                    ctab[other], atab[own], preferred_element_type=jnp.float32
                )
                weight = jnp.exp2(jnp.minimum(spread, 0.0))
                upper = weight.astype(jnp.bfloat16)
                lower = (weight - upper.astype(jnp.float32)).astype(jnp.bfloat16)
                rows = htab[other]
                parts.append(
                    jnp.dot(rows, upper, preferred_element_type=jnp.float32)
                    + jnp.dot(rows, lower, preferred_element_type=jnp.float32)
                )
                owners.append(own)
            for own, part in zip(owners, parts):
                acc[own] += part
            return 0

        lax.fori_loop(0, (live + UNROLL - 1) // UNROLL, some, 0)

    def force_of(block, pull, x):
        got = acc[block]
        moved = got[:8] + got[8:]
        moved = moved + pltpu.roll(moved, 4, 0)
        weight = total4(jnp.where(fourth, moved, 0.0))
        pair = (x * ROOT * weight - moved) * (PAIR_EPS / ROOT)
        pair = jnp.where(fourth, 0.0, pair)
        return pair - (pull[0] * w0s[block] + pull[1] * w1s[block])

    atab[slabs * blocks] = jnp.zeros((32, BLK), jnp.bfloat16)

    def step(number, sums):
        for slab in range(slabs):
            tiles(slab)
        pull = pulls(sums)
        kick = jnp.where(number == 0, jnp.float32(0.5 * DT), jnp.float32(DT))

        def advance(block, carry):
            x = xs[block]
            v = vs[block] + kick * ms[block] * force_of(block, pull, x)
            x = x + DT * v
            xs[block] = x
            vs[block] = v
            tables(block, x)
            return carry[0] + w0s[block] * x, carry[1] + w1s[block] * x

        zero = jnp.zeros((8, BLK), jnp.float32)
        return lax.fori_loop(0, slabs * blocks, advance, (zero, zero))

    sums = lax.fori_loop(0, STEPS, step, sums)
    tiles(0)
    pull = pulls(sums)

    order = stat_refs[0][7:8, :].astype(jnp.int32)
    high, low = order // BLK, order % BLK
    size = blocks * BLK
    place = lax.broadcasted_iota(jnp.int32, (blocks, size), 1)
    hit_high = lax.broadcasted_iota(jnp.int32, (blocks, size), 0) == high
    hit_low = lax.broadcasted_iota(jnp.int32, (BLK, size), 0) == low
    left = jnp.concatenate(
        [
            jnp.where(hit_high, place // BLK, 0).astype(jnp.float32),
            jnp.where(hit_high, place % BLK, 0).astype(jnp.float32),
        ],
        0,
    ).astype(jnp.bfloat16)
    right = jnp.where(hit_low, 1.0, 0.0).astype(jnp.bfloat16)
    inv[...] = lax.dot_general(
        left, right, (((1,), (1,)), ((), ())), preferred_element_type=jnp.float32
    ).astype(jnp.int32)

    for block in range(blocks):
        x = xs[block]
        force = force_of(block, pull, x)
        v = vs[block] + (0.5 * DT) * ms[block] * force
        packed[0, :, block * BLK : (block + 1) * BLK] = jnp.where(row < 4, x, v)
        packed[1, :, block * BLK : (block + 1) * BLK] = force

    def give(t, _):
        high = jnp.broadcast_to(inv[pl.ds(t, 1), :], (8, BLK))
        low = jnp.broadcast_to(inv[pl.ds(blocks + t, 1), :], (8, BLK))
        first = jnp.zeros((8, BLK), jnp.float32)
        second = jnp.zeros((8, BLK), jnp.float32)
        for b in range(blocks):
            here = high == b
            first = jnp.where(here, lanes_from(packed[0, :, b * BLK : (b + 1) * BLK], low), first)
            second = jnp.where(here, lanes_from(packed[1, :, b * BLK : (b + 1) * BLK], low), second)
        at = pl.ds(pl.multiple_of(t * BLK, BLK), BLK)
        x_out[:, at] = first[0:3]
        v_out[:, at] = first[4:7]
        f_out[:, at] = second[0:3]
        return 0

    lax.fori_loop(0, blocks, give, 0)


def partner(value, flip_row, flip_col):
    rows, cols = lax.axis_size("wrow"), lax.axis_size("wcol")
    pairs = [
        (r * cols + c, (r ^ flip_row) * cols + (c ^ flip_col))
        for r in range(rows)
        for c in range(cols)
    ]
    return lax.ppermute(value, ("wrow", "wcol"), pairs)


def round_dom(value):
    count = lax.axis_size("dom")
    return [value] + [
        lax.ppermute(value, "dom", [((i + s) % count, i) for i in range(count)])
        for s in range(1, count)
    ]


def per_device(
    positions,
    velocities,
    inv_mass,
    cv_weight,
    stiffness,
    centers,
    block_order,
    pair_count,
    pair_own,
    pair_other,
    accept_row,
    accept_col,
):
    size = block_order.shape[0]
    blocks = size // BLK
    slots = pair_own.shape[1]
    slabs = lax.axis_size("dom")
    listed = -(-slots // UNROLL) * UNROLL

    aux = jnp.concatenate([centers[0, 0], accept_row[0].astype(jnp.float32)])
    aux = jnp.pad(aux, (0, size - 3))[None]
    nothing = jnp.zeros((1, size), jnp.float32)
    state = jnp.concatenate([positions[0, 0], aux, velocities[0, 0], nothing], 0)
    by_row = partner(state, 1, 0)
    by_col = partner(state, 0, 1)
    by_both = partner(state, 1, 1)
    far = jnp.where(by_col[3, 2] == 1.0, by_both, by_col)
    near = jnp.where(accept_row[0, 0] == 1, by_row, state)
    state = jnp.where(accept_col[0, 0] == 1, far, near)
    dyn = round_dom(state)

    fixed = jnp.concatenate(
        [cv_weight[0], inv_mass[None], cv_weight[1], block_order.astype(jnp.float32)[None]], 0
    )
    stat = round_dom(fixed)
    lists = jnp.concatenate(
        [
            jnp.pad(pair_own, ((0, 0), (0, listed - slots))),
            jnp.pad(pair_other, ((0, 0), (0, listed - slots))),
            pair_count[None],
        ],
        1,
    )
    lists = jnp.concatenate(round_dom(lists), 0)
    own, other, count = lists[:, :listed], lists[:, listed : 2 * listed], lists[:, 2 * listed]

    whole_vmem = pl.BlockSpec(memory_space=pltpu.VMEM)
    smem = pl.BlockSpec(memory_space=pltpu.SMEM)
    total = slabs * blocks
    part = lambda: pltpu.VMEM((total, 8, BLK), jnp.float32)
    outs = pl.pallas_call(
        functools.partial(kernel, slabs, blocks, slots),
        out_shape=[jax.ShapeDtypeStruct((3, size), jnp.float32)] * 3,
        in_specs=[smem] * 4 + [whole_vmem] * (2 * slabs),
        out_specs=[whole_vmem] * 3,
        scratch_shapes=[
            part(),
            part(),
            part(),
            part(),
            part(),
            pltpu.VMEM((total + 1, 16, BLK), jnp.float32),
            pltpu.VMEM((total + 1, 32, BLK), jnp.bfloat16),
            pltpu.VMEM((total, BLK, 32), jnp.bfloat16),
            pltpu.VMEM((total, 16, BLK), jnp.bfloat16),
            pltpu.VMEM((2 * blocks, BLK), jnp.int32),
            pltpu.VMEM((2, 8, size), jnp.float32),
        ],
    )(own, other, count, stiffness, *dyn, *stat)
    return tuple(out[None, None] for out in outs)


def solution(mesh):
    placed = (
        P("wrow", "wcol", None, "dom"),
        P("wrow", "wcol", None, "dom"),
        P("dom"),
        P(None, None, "dom"),
        P(),
        P("wrow", "wcol", None),
        P("dom"),
        P("dom"),
        P("dom", None),
        P("dom", None),
        P("wrow", "wcol"),
        P("wrow", "wcol"),
    )
    return jax.shard_map(
        per_device,
        mesh=mesh,
        in_specs=placed,
        out_specs=(P("wrow", "wcol", None, "dom"),) * 3,
        check_vma=False,
    )
```

```python
import functools
import math

import jax
import jax.numpy as jnp
from jax import lax
from jax.experimental import pallas as pl
from jax.experimental.pallas import tpu as pltpu
from jax.sharding import PartitionSpec as P

BLK = 128
STEPS = 3
PAIR_EPS = 0.015625
DT = 0.1
UNROLL = 4
BRING = 2
PASS = 8
ROOT = math.sqrt(math.log2(math.e))


def rounded(x):
    return x.astype(jnp.bfloat16).astype(jnp.float32)


def lanes_from(source, low):
    return jnp.take_along_axis(source, low, axis=1, mode="promise_in_bounds")


def kernel(slabs, blocks, slots, *refs):
    own_ref, other_ref, count_ref, stiff_ref = refs[:4]
    dyn_refs = refs[4 : 4 + slabs]
    stat_refs = refs[4 + slabs : 4 + 2 * slabs]
    x_out, v_out, f_out = refs[4 + 2 * slabs : 7 + 2 * slabs]
    xs, vs, ms, w0s, w1s, acc, atab, ctab, htab, spread, inv, packed = refs[7 + 2 * slabs :]
    total = slabs * blocks
    row = lax.broadcasted_iota(jnp.int32, (8, BLK), 0)
    fourth = (row == 3) | (row == 7)
    centre = [dyn_refs[0][3:4, k : k + 1] for k in range(2)]

    def doubled(value):
        turned = pltpu.roll(value, 4, 0)
        return jnp.where(row < 4, value, turned), jnp.where(row < 4, turned, value)

    def total4(value):
        value = value + pltpu.roll(value, 1, 0)
        return value + pltpu.roll(value, 2, 0)

    def tables(group):
        made = []
        for block, x in group:
            scaled = jnp.where(fourth, 0.0, x * ROOT)
            half = -0.5 * total4(scaled * scaled)
            base = jnp.where(fourth, half, scaled)
            s1 = rounded(base)
            rest = base - s1
            s2 = rounded(rest)
            s3 = rest - s2
            one = jnp.float32(1.0)
            zero = jnp.zeros_like(x)
            a0 = jnp.where(row == 7, s2, s1)
            a1 = jnp.where(row == 3, s3, jnp.where(row == 7, one, s2))
            a2 = jnp.where(row < 3, s1, jnp.where(fourth, one, s3))
            c0 = jnp.where(row < 3, s1, jnp.where(fourth, one, s2))
            c1 = jnp.where((row < 3) | (row == 7), s1, jnp.where(row == 3, one, s2))
            c2 = jnp.where((row < 3) | (row == 7), s3, jnp.where(row == 3, s2, s1))
            h0 = jnp.where(row == 3, one, jnp.where(row == 7, 0.0, jnp.where(row < 4, s1, s2)))
            h1 = jnp.where(row < 3, s3, 0.0)
            ours = jnp.concatenate([a0, a1, a2, zero], 0).astype(jnp.bfloat16)
            theirs = jnp.concatenate([c0, c1, c2, zero], 0).T.astype(jnp.bfloat16)
            heads = jnp.concatenate([h0, h1], 0).astype(jnp.bfloat16)
            made.append((block, ours, theirs, heads))
        for block, ours, theirs, heads in made:
            atab[block] = ours
            ctab[block] = theirs
            htab[block, :, :BLK] = heads
            htab[block, :, BLK:] = heads
            acc[block] = jnp.zeros((16, BLK), jnp.float32)

    def whole(value):
        return jnp.sum(jnp.sum(value, axis=0, keepdims=True), axis=1, keepdims=True)

    zero = jnp.zeros((8, BLK), jnp.float32)
    sums = (zero, zero)
    for slab in range(slabs):

        def bring(pair, carry, slab=slab):
            dyn, stat = dyn_refs[slab], stat_refs[slab]
            group = []
            for u in range(BRING):
                t = pair * BRING + u
                first = pl.multiple_of(t * BLK, BLK)
                index = stat[7:8, pl.ds(first, BLK)].astype(jnp.int32)
                index = jnp.broadcast_to(index, (8, BLK))
                high, low = index // BLK, index % BLK
                state = jnp.zeros((8, BLK), jnp.float32)
                fixed = jnp.zeros((8, BLK), jnp.float32)
                for b in range(blocks):
                    here = high == b
                    at = slice(b * BLK, (b + 1) * BLK)
                    state = jnp.where(here, lanes_from(dyn[:, at], low), state)
                    fixed = jnp.where(here, lanes_from(stat[:, at], low), fixed)
                x, v = doubled(state)
                w0, w1 = doubled(jnp.where(fourth, 0.0, fixed))
                m = jnp.broadcast_to(fixed[3:4], (8, BLK))
                group.append((slab * blocks + t, x, v, w0, w1, m))
            for block, x, v, w0, w1, m in group:
                xs[block] = x
                vs[block] = v
                w0s[block] = w0
                w1s[block] = w1
                ms[block] = m
                carry = carry[0] + w0 * x, carry[1] + w1 * x
            tables([(block, x) for block, x, *_ in group])
            return carry

        sums = lax.fori_loop(0, blocks // BRING, bring, sums)

    def pulls(pair):
        return [stiff_ref[k] * (0.5 * whole(pair[k]) - centre[k]) for k in range(2)]

    lives = [count_ref[slab] for slab in range(slabs)]
    ends = []
    for slab in range(slabs):
        groups = (lives[slab] + UNROLL - 1) // UNROLL
        ends.append(groups + (ends[-1] if slab else 0))

    def tiles(limit):
        def entries(group):
            slab, start, live = jnp.int32(0), jnp.int32(0), lives[0]
            for k in range(1, slabs):
                past = group >= ends[k - 1]
                slab = jnp.where(past, k, slab)
                start = jnp.where(past, ends[k - 1], start)
                live = jnp.where(past, lives[k], live)
            live = jnp.where(group < limit, live, 0)
            found = []
            for u in range(UNROLL):
                p = (group - start) * UNROLL + u
                inside = p < live
                q = jnp.where(inside, p, 0)
                own = jnp.where(inside, own_ref[slab, q] + slab * blocks, total)
                other = other_ref[slab, q] + (slab - 1) * blocks
                other = jnp.where(other < 0, other + total, other)
                other = jnp.where(other >= total, other - total, other)
                found.append((own, other))
            return found

        def spreads(found):
            return [
                jnp.dot(ctab[other], atab[own], preferred_element_type=jnp.float32)
                for own, other in found
            ]

        def some(group, carry):
            found, earlier, parts = carry
            following = entries(group + 1)
            later = spreads(following)
            new = []
            for u in range(UNROLL):
                weight = jnp.exp2(jnp.minimum(spread[u], 0.0))
                upper = weight.astype(jnp.bfloat16)
                lower = (weight - upper.astype(jnp.float32)).astype(jnp.bfloat16)
                both = jnp.concatenate([upper, lower], 0)
                new.append(
                    jnp.dot(htab[found[u][1]], both, preferred_element_type=jnp.float32)
                )
            for own, part in zip(earlier, parts):
                acc[own] += part
            for u in range(UNROLL):
                spread[u] = later[u]
            return following, [own for own, _ in found], new

        found = entries(jnp.int32(0))
        for u, value in enumerate(spreads(found)):
            spread[u] = value
        nobody = [jnp.int32(total)] * UNROLL
        nothing = [jnp.zeros((16, BLK), jnp.float32)] * UNROLL
        _, earlier, parts = lax.fori_loop(0, limit, some, (found, nobody, nothing))
        for own, part in zip(earlier, parts):
            acc[own] += part

    def force_of(block, pull, x):
        got = acc[block]
        moved = got[:8] + got[8:]
        moved = moved + pltpu.roll(moved, 4, 0)
        weight = total4(jnp.where(fourth, moved, 0.0))
        pair = (x * ROOT * weight - moved) * (PAIR_EPS / ROOT)
        pair = jnp.where(fourth, 0.0, pair)
        return pair - (pull[0] * w0s[block] + pull[1] * w1s[block])

    atab[total] = jnp.zeros((32, BLK), jnp.bfloat16)

    def step(number, sums):
        tiles(ends[-1])
        pull = pulls(sums)
        kick = jnp.where(number == 0, jnp.float32(0.5 * DT), jnp.float32(DT))

        def advance(group, carry):
            moved = []
            for u in range(PASS):
                block = group * PASS + u
                x = xs[block]
                v = vs[block] + kick * ms[block] * force_of(block, pull, x)
                x = x + DT * v
                moved.append((block, x, v))
                carry = carry[0] + w0s[block] * x, carry[1] + w1s[block] * x
            for block, x, v in moved:
                xs[block] = x
                vs[block] = v
            tables([(block, x) for block, x, _ in moved])
            return carry

        return lax.fori_loop(0, total // PASS, advance, (zero, zero))

    sums = lax.fori_loop(0, STEPS, step, sums)
    tiles(ends[0])
    pull = pulls(sums)

    order = stat_refs[0][7:8, :].astype(jnp.int32)
    high, low = order // BLK, order % BLK
    size = blocks * BLK
    place = lax.broadcasted_iota(jnp.int32, (blocks, size), 1)
    hit_high = lax.broadcasted_iota(jnp.int32, (blocks, size), 0) == high
    hit_low = lax.broadcasted_iota(jnp.int32, (BLK, size), 0) == low
    left = jnp.concatenate(
        [
            jnp.where(hit_high, place // BLK, 0).astype(jnp.float32),
            jnp.where(hit_high, place % BLK, 0).astype(jnp.float32),
        ],
        0,
    ).astype(jnp.bfloat16)
    right = jnp.where(hit_low, 1.0, 0.0).astype(jnp.bfloat16)
    inv[...] = lax.dot_general(
        left, right, (((1,), (1,)), ((), ())), preferred_element_type=jnp.float32
    ).astype(jnp.int32)

    for block in range(blocks):
        x = xs[block]
        force = force_of(block, pull, x)
        v = vs[block] + (0.5 * DT) * ms[block] * force
        packed[0, :, block * BLK : (block + 1) * BLK] = jnp.where(row < 4, x, v)
        packed[1, :, block * BLK : (block + 1) * BLK] = force

    def give(pair, _):
        done = []
        for u in range(BRING):
            t = pair * BRING + u
            high = jnp.broadcast_to(inv[pl.ds(t, 1), :], (8, BLK))
            low = jnp.broadcast_to(inv[pl.ds(blocks + t, 1), :], (8, BLK))
            first, second = zero, zero
            for b in range(blocks):
                here = high == b
                at = slice(b * BLK, (b + 1) * BLK)
                first = jnp.where(here, lanes_from(packed[0, :, at], low), first)
                second = jnp.where(here, lanes_from(packed[1, :, at], low), second)
            done.append((pl.ds(pl.multiple_of(t * BLK, BLK), BLK), first, second))
        for at, first, second in done:
            x_out[:, at] = first[0:3]
            v_out[:, at] = first[4:7]
            f_out[:, at] = second[0:3]
        return 0

    lax.fori_loop(0, blocks // BRING, give, 0)


def partner(value, flip_row, flip_col):
    rows, cols = lax.axis_size("wrow"), lax.axis_size("wcol")
    pairs = [
        (r * cols + c, (r ^ flip_row) * cols + (c ^ flip_col))
        for r in range(rows)
        for c in range(cols)
    ]
    return lax.ppermute(value, ("wrow", "wcol"), pairs)


def round_dom(value):
    count = lax.axis_size("dom")
    return [value] + [
        lax.ppermute(value, "dom", [((i + s) % count, i) for i in range(count)])
        for s in range(1, count)
    ]


def per_device(
    positions,
    velocities,
    inv_mass,
    cv_weight,
    stiffness,
    centers,
    block_order,
    pair_count,
    pair_own,
    pair_other,
    accept_row,
    accept_col,
):
    size = block_order.shape[0]
    blocks = size // BLK
    slots = pair_own.shape[1]
    slabs = lax.axis_size("dom")
    listed = -(-slots // UNROLL) * UNROLL

    aux = jnp.concatenate([centers[0, 0], accept_row[0].astype(jnp.float32)])
    aux = jnp.pad(aux, (0, size - 3))[None]
    nothing = jnp.zeros((1, size), jnp.float32)
    state = jnp.concatenate([positions[0, 0], aux, velocities[0, 0], nothing], 0)
    by_row = partner(state, 1, 0)
    by_col = partner(state, 0, 1)
    by_both = partner(state, 1, 1)
    far = jnp.where(by_col[3, 2] == 1.0, by_both, by_col)
    near = jnp.where(accept_row[0, 0] == 1, by_row, state)
    state = jnp.where(accept_col[0, 0] == 1, far, near)
    dyn = round_dom(state)

    fixed = jnp.concatenate(
        [cv_weight[0], inv_mass[None], cv_weight[1], block_order.astype(jnp.float32)[None]], 0
    )
    stat = round_dom(fixed)
    lists = jnp.concatenate(
        [
            jnp.pad(pair_own, ((0, 0), (0, listed - slots))),
            jnp.pad(pair_other, ((0, 0), (0, listed - slots))),
            pair_count[None],
        ],
        1,
    )
    lists = jnp.concatenate(round_dom(lists), 0)
    own, other, count = lists[:, :listed], lists[:, listed : 2 * listed], lists[:, 2 * listed]

    whole_vmem = pl.BlockSpec(memory_space=pltpu.VMEM)
    smem = pl.BlockSpec(memory_space=pltpu.SMEM)
    total = slabs * blocks
    part = lambda: pltpu.VMEM((total, 8, BLK), jnp.float32)
    outs = pl.pallas_call(
        functools.partial(kernel, slabs, blocks, slots),
        out_shape=[jax.ShapeDtypeStruct((3, size), jnp.float32)] * 3,
        in_specs=[smem] * 4 + [whole_vmem] * (2 * slabs),
        out_specs=[whole_vmem] * 3,
        scratch_shapes=[
            part(),
            part(),
            part(),
            part(),
            part(),
            pltpu.VMEM((total + 1, 16, BLK), jnp.float32),
            pltpu.VMEM((total + 1, 32, BLK), jnp.bfloat16),
            pltpu.VMEM((total, BLK, 32), jnp.bfloat16),
            pltpu.VMEM((total, 16, 2 * BLK), jnp.bfloat16),
            pltpu.VMEM((UNROLL, BLK, BLK), jnp.float32),
            pltpu.VMEM((2 * blocks, BLK), jnp.int32),
            pltpu.VMEM((2, 8, size), jnp.float32),
        ],
    )(own, other, count, stiffness, *dyn, *stat)
    return tuple(out[None, None] for out in outs)


def solution(mesh):
    placed = (
        P("wrow", "wcol", None, "dom"),
        P("wrow", "wcol", None, "dom"),
        P("dom"),
        P(None, None, "dom"),
        P(),
        P("wrow", "wcol", None),
        P("dom"),
        P("dom"),
        P("dom", None),
        P("dom", None),
        P("wrow", "wcol"),
        P("wrow", "wcol"),
    )
    return jax.shard_map(
        per_device,
        mesh=mesh,
        in_specs=placed,
        out_specs=(P("wrow", "wcol", None, "dom"),) * 3,
        check_vma=False,
    )
```

```python
import functools
import math

import jax
import jax.numpy as jnp
from jax import lax
from jax.experimental import pallas as pl
from jax.experimental.pallas import tpu as pltpu
from jax.sharding import PartitionSpec as P

BLK = 128
STEPS = 3
PAIR_EPS = 0.015625
DT = 0.1
UNROLL = 16
PASS = 16
SMALL_VMEM = 4 << 20
MAIN_VMEM = 24 << 20
ROOT = math.sqrt(math.log2(math.e))


def rounded(x):
    return x.astype(jnp.bfloat16).astype(jnp.float32)


def lanes_from(source, low):
    return jnp.take_along_axis(source, low, axis=1, mode="promise_in_bounds")


def sub_row():
    return lax.broadcasted_iota(jnp.int32, (8, BLK), 0)


def is_fourth():
    row = sub_row()
    return (row == 3) | (row == 7)


def total4(value):
    value = value + pltpu.roll(value, 1, 0)
    return value + pltpu.roll(value, 2, 0)


def whole(value):
    return jnp.sum(jnp.sum(value, axis=0, keepdims=True), axis=1, keepdims=True)


def span(block):
    return pl.ds(pl.multiple_of(block * BLK, BLK), BLK)


def reordered(high, low, rows):
    found = []
    for b, group in enumerate(rows):
        here = high == b
        for k, row in enumerate(group):
            moved = lanes_from(jnp.broadcast_to(row, high.shape), low)
            if b:
                found[k] = jnp.where(here, moved, found[k])
            else:
                found.append(moved)
    return found


def state_kernel(blocks, centers, pos, vel, mass, order, out):
    index = order[...]
    high, low = index // BLK, index % BLK
    refs = [(pos, 0), (pos, 1), (pos, 2), (mass, 0), (vel, 0), (vel, 1), (vel, 2)]
    rows = [
        [ref[k * blocks + b : k * blocks + b + 1, :] for ref, k in refs] for b in range(blocks)
    ]
    for k, value in enumerate(reordered(high, low, rows)):
        out[k * blocks : (k + 1) * blocks, :] = value
    lane = lax.broadcasted_iota(jnp.int32, (blocks, BLK), 1)
    out[7 * blocks :, :] = jnp.where(lane == 0, centers[0, 0], centers[0, 1])


def weight_kernel(blocks, slots, count, cv, order, own, other, out):
    index = order[...]
    high, low = index // BLK, index % BLK
    rows = [
        [cv[pl.ds((c * blocks + b) * 2 + k, 1), :] for k in range(2) for c in range(3)]
        for b in range(blocks)
    ]
    out[3 * blocks : 4 * blocks, :] = jnp.zeros((blocks, BLK), jnp.float32)
    for k, value in enumerate(reordered(high, low, rows)):
        k = k + k // 3
        out[k * blocks : (k + 1) * blocks, :] = value
    out[7 * blocks :, :] = jnp.zeros((blocks, BLK), jnp.float32) + count[0].astype(jnp.float32)
    lines = -(-slots // BLK)
    for j in range(lines):
        wide = min(BLK, slots - j * BLK)
        at = slice(j * BLK, j * BLK + wide)
        mine = 7 * blocks + 1 + j
        out[mine : mine + 1, 0:wide] = own[0:1, at].astype(jnp.float32)
        out[mine + lines : mine + lines + 1, 0:wide] = other[0:1, at].astype(jnp.float32)


def inverse_kernel(blocks, order, inv):
    size = blocks * BLK
    listed = jnp.concatenate([order[b : b + 1, :] for b in range(blocks)], 1)
    high, low = listed // BLK, listed % BLK
    place = lax.broadcasted_iota(jnp.int32, (blocks, size), 1)
    hit_high = lax.broadcasted_iota(jnp.int32, (blocks, size), 0) == high
    hit_low = lax.broadcasted_iota(jnp.int32, (BLK, size), 0) == low
    left = jnp.concatenate(
        [
            jnp.where(hit_high, place // BLK, 0).astype(jnp.float32),
            jnp.where(hit_high, place % BLK, 0).astype(jnp.float32),
        ],
        0,
    ).astype(jnp.bfloat16)
    right = jnp.where(hit_low, 1.0, 0.0).astype(jnp.bfloat16)
    inv[...] = lax.dot_general(
        left, right, (((1,), (1,)), ((), ())), preferred_element_type=jnp.float32
    ).astype(jnp.int32)


class Pairs:
    def __init__(self, slabs, blocks, slots, lists, acc, atab, ctab, htab, spread):
        self.slabs, self.blocks, self.total = slabs, blocks, slabs * blocks
        self.slots, self.lists = slots, lists
        self.acc, self.atab, self.ctab, self.htab = acc, atab, ctab, htab
        self.spread = spread
        self.lines = -(-slots // BLK)
        self.lives = [self.number(slab, 0, 0) for slab in range(slabs)]
        self.ends = []
        for slab in range(slabs):
            groups = (self.lives[slab] + UNROLL - 1) // UNROLL
            self.ends.append(groups + (self.ends[-1] if slab else 0))
        atab[self.total] = jnp.zeros((32, BLK), jnp.bfloat16)

    def number(self, slab, line, at):
        if self.lines > 1:
            line, at = line + at // BLK, at % BLK
        return self.lists[slab, line, at].astype(jnp.int32)

    def tables(self, group):
        row, fourth = sub_row(), is_fourth()
        made = []
        for block, x in group:
            scaled = jnp.where(fourth, 0.0, x * ROOT)
            half = -0.5 * total4(scaled * scaled)
            base = jnp.where(fourth, half, scaled)
            s1 = rounded(base)
            rest = base - s1
            s2 = rounded(rest)
            s3 = rest - s2
            one = jnp.float32(1.0)
            zero = jnp.zeros_like(x)
            a0 = jnp.where(row == 7, s2, s1)
            a1 = jnp.where(row == 3, s3, jnp.where(row == 7, one, s2))
            a2 = jnp.where(row < 3, s1, jnp.where(fourth, one, s3))
            c0 = jnp.where(row < 3, s1, jnp.where(fourth, one, s2))
            c1 = jnp.where((row < 3) | (row == 7), s1, jnp.where(row == 3, one, s2))
            c2 = jnp.where((row < 3) | (row == 7), s3, jnp.where(row == 3, s2, s1))
            h0 = jnp.where(row == 3, one, jnp.where(row == 7, 0.0, jnp.where(row < 4, s1, s2)))
            h1 = jnp.where(row < 3, s3, 0.0)
            ours = jnp.concatenate([a0, a1, a2, zero], 0).astype(jnp.bfloat16)
            theirs = jnp.concatenate([c0, c1, c2, zero], 0).T.astype(jnp.bfloat16)
            heads = jnp.concatenate([h0, h1], 0).astype(jnp.bfloat16)
            made.append((block, ours, theirs, heads))
        for block, ours, theirs, heads in made:
            self.atab[block] = ours
            self.ctab[block] = theirs
            self.htab[block, :, :BLK] = heads
            self.htab[block, :, BLK:] = heads
            self.acc[block] = jnp.zeros((16, BLK), jnp.float32)

    def entries(self, group, limit):
        slab, start, live = jnp.int32(0), jnp.int32(0), self.lives[0]
        for k in range(1, self.slabs):
            past = group >= self.ends[k - 1]
            slab = jnp.where(past, k, slab)
            start = jnp.where(past, self.ends[k - 1], start)
            live = jnp.where(past, self.lives[k], live)
        live = jnp.where(group < limit, live, 0)
        found = []
        for u in range(UNROLL):
            p = (group - start) * UNROLL + u
            inside = p < live
            q = jnp.where(inside, p, 0)
            own = jnp.where(inside, self.number(slab, 1, q) + slab * self.blocks, self.total)
            other = self.number(slab, 1 + self.lines, q) + (slab - 1) * self.blocks
            other = jnp.where(other < 0, other + self.total, other)
            other = jnp.where(other >= self.total, other - self.total, other)
            found.append((own, other))
        return found

    def spreads(self, found):
        return [
            jnp.dot(self.ctab[other], self.atab[own], preferred_element_type=jnp.float32)
            for own, other in found
        ]

    def run(self, limit):
        def some(group, carry):
            found, earlier, parts = carry
            following = self.entries(group + 1, limit)
            later = self.spreads(following)
            new = []
            for u in range(UNROLL):
                weight = jnp.exp2(jnp.minimum(self.spread[u], 0.0))
                upper = weight.astype(jnp.bfloat16)
                lower = (weight - upper.astype(jnp.float32)).astype(jnp.bfloat16)
                both = jnp.concatenate([upper, lower], 0)
                new.append(
                    jnp.dot(self.htab[found[u][1]], both, preferred_element_type=jnp.float32)
                )
            for own, part in zip(earlier, parts):
                self.acc[own] += part
            for u in range(UNROLL):
                self.spread[u] = later[u]
            return following, [own for own, _ in found], new

        found = self.entries(jnp.int32(0), limit)
        for u, value in enumerate(self.spreads(found)):
            self.spread[u] = value
        nobody = [jnp.int32(self.total)] * UNROLL
        nothing = [jnp.zeros((16, BLK), jnp.float32)] * UNROLL
        _, earlier, parts = lax.fori_loop(0, limit, some, (found, nobody, nothing))
        for own, part in zip(earlier, parts):
            self.acc[own] += part

    def force(self, got, x):
        fourth = is_fourth()
        moved = got[:8] + got[8:]
        moved = moved + pltpu.roll(moved, 4, 0)
        weight = total4(jnp.where(fourth, moved, 0.0))
        pair = (x * ROOT * weight - moved) * (PAIR_EPS / ROOT)
        return jnp.where(fourth, 0.0, pair)


def steps_kernel(slabs, blocks, slots, *refs):
    stiff_ref, inv = refs[:2]
    state_refs = refs[2 : 2 + slabs]
    fixed_refs = refs[2 + slabs : 2 + 2 * slabs]
    x_out, v_out, f_out = refs[2 + 2 * slabs : 5 + 2 * slabs]
    xs, vs, ms, w0s, w1s, packed, lists, sem, *rest = refs[5 + 2 * slabs :]
    acc = rest[0]
    copies = [
        pltpu.make_async_copy(
            fixed.at[pl.ds(7 * blocks, lists.shape[1]), :], lists.at[k], sem.at[k]
        )
        for k, fixed in enumerate(fixed_refs)
    ]
    for copy in copies:
        copy.start()
    total = slabs * blocks
    row, fourth = sub_row(), is_fourth()
    centre = [state_refs[0][7 * blocks : 7 * blocks + 1, k : k + 1] for k in range(2)]
    zero = jnp.zeros((8, BLK), jnp.float32)

    def strided(ref, t):
        return ref[pl.ds(t, 8, stride=blocks), :]

    for copy in copies:
        copy.wait()
    work = Pairs(slabs, blocks, slots, lists, *rest)

    sums = (zero, zero)
    for slab in range(slabs):

        def load(group, carry, slab=slab):
            done = []
            for u in range(PASS):
                t = group * PASS + u
                state = strided(state_refs[slab], t)
                m = jnp.broadcast_to(state[3:4], (8, BLK))
                state = jnp.where(fourth, 0.0, state)
                turned = pltpu.roll(state, 4, 0)
                x = jnp.where(row < 4, state, turned)
                v = jnp.where(row < 4, turned, state)
                w = jnp.where(fourth, 0.0, strided(fixed_refs[slab], t))
                turned = pltpu.roll(w, 4, 0)
                w0 = jnp.where(row < 4, w, turned)
                w1 = jnp.where(row < 4, turned, w)
                carry = carry[0] + w0 * x, carry[1] + w1 * x
                done.append((slab * blocks + t, x, v, m, w0, w1))
            for block, x, v, m, w0, w1 in done:
                xs[block] = x
                vs[block] = v
                ms[block] = m
                w0s[block] = w0
                w1s[block] = w1
            work.tables([(block, x) for block, x, *_ in done])
            return carry

        sums = lax.fori_loop(0, blocks // PASS, load, sums)

    def pulls(pair):
        return [stiff_ref[k] * (0.5 * whole(pair[k]) - centre[k]) for k in range(2)]

    def step(number, sums):
        work.run(work.ends[-1])
        pull = pulls(sums)
        kick = jnp.where(number == 0, jnp.float32(0.5 * DT), jnp.float32(DT))

        def some(group, carry):
            moved = []
            for u in range(PASS):
                block = group * PASS + u
                x = xs[block]
                force = work.force(acc[block], x) - (pull[0] * w0s[block] + pull[1] * w1s[block])
                v = vs[block] + kick * ms[block] * force
                x = x + DT * v
                moved.append((block, x, v))
                carry = carry[0] + w0s[block] * x, carry[1] + w1s[block] * x
            for block, x, v in moved:
                xs[block] = x
                vs[block] = v
            work.tables([(block, x) for block, x, _ in moved])
            return carry

        return lax.fori_loop(0, total // PASS, some, (zero, zero))

    sums = lax.fori_loop(0, STEPS, step, sums)
    work.run(work.ends[0])
    pull = pulls(sums)

    for block in range(blocks):
        x = xs[block]
        force = work.force(acc[block], x) - (pull[0] * w0s[block] + pull[1] * w1s[block])
        v = vs[block] + (0.5 * DT) * ms[block] * force
        packed[block, 0:8] = jnp.where(row < 4, x, v)
        packed[block, 8:16] = force
    rows = [
        [packed[b, k : k + 1, :] for k in (0, 1, 2, 4, 5, 6, 8, 9, 10)] for b in range(blocks)
    ]
    found = reordered(inv[:blocks, :], inv[blocks:, :], rows)
    for k, value in enumerate(found):
        out = (x_out, v_out, f_out)[k // 3]
        k = k % 3
        out[k * blocks : (k + 1) * blocks, :] = value


def swapped(value, axis, accept):
    pairs = [(i, i ^ 1) for i in range(lax.axis_size(axis))]
    return jnp.where(accept == 1, lax.ppermute(value, axis, pairs), value)


def round_dom(value):
    count = lax.axis_size("dom")
    return [value] + [
        lax.ppermute(value, "dom", [((i + s) % count, i) for i in range(count)])
        for s in range(1, count)
    ]


def per_device(
    positions,
    velocities,
    inv_mass,
    cv_weight,
    stiffness,
    centers,
    block_order,
    pair_count,
    pair_own,
    pair_other,
    accept_row,
    accept_col,
):
    size = block_order.shape[0]
    blocks = size // BLK
    slots = pair_own.shape[1]
    slabs = lax.axis_size("dom")
    total = slabs * blocks
    vmem = pl.BlockSpec(memory_space=pltpu.VMEM)
    smem = pl.BlockSpec(memory_space=pltpu.SMEM)
    floats = jnp.float32
    payload = jax.ShapeDtypeStruct((8 * blocks, BLK), floats)

    def lines(value):
        return value.reshape(-1, BLK)

    def small(flops):
        return dict(
            compiler_params=pltpu.CompilerParams(vmem_limit_bytes=SMALL_VMEM),
            cost_estimate=pl.CostEstimate(
                flops=flops, bytes_accessed=1 << 17, transcendentals=0
            ),
        )

    order = lines(block_order)
    state = pl.pallas_call(
        functools.partial(state_kernel, blocks),
        out_shape=payload,
        in_specs=[smem] + [vmem] * 4,
        out_specs=vmem,
        **small(1 << 24),
    )(centers[0], lines(positions), lines(velocities), lines(inv_mass), order)
    weights = cv_weight.reshape(2, 3, blocks, BLK).transpose(1, 2, 0, 3).reshape(-1, BLK)
    fixed = pl.pallas_call(
        functools.partial(weight_kernel, blocks, slots),
        out_shape=payload,
        in_specs=[smem] + [vmem] * 4,
        out_specs=vmem,
        **small(1 << 24),
    )(pair_count, weights, order, pair_own, pair_other)
    inverse = pl.pallas_call(
        functools.partial(inverse_kernel, blocks),
        out_shape=jax.ShapeDtypeStruct((2 * blocks, BLK), jnp.int32),
        in_specs=[vmem],
        out_specs=vmem,
        **small(1 << 24),
    )(order)

    state = swapped(state, "wrow", accept_row[0, 0])
    state = swapped(state, "wcol", accept_col[0, 0])
    fixeds = round_dom(fixed)
    states = round_dom(state)

    part = pltpu.VMEM((total, 8, BLK), floats)
    outs = pl.pallas_call(
        functools.partial(steps_kernel, slabs, blocks, slots),
        out_shape=[jax.ShapeDtypeStruct((3 * blocks, BLK), floats)] * 3,
        in_specs=[smem] + [vmem] * (1 + 2 * slabs),
        out_specs=[vmem] * 3,
        scratch_shapes=[part] * 5
        + [
            pltpu.VMEM((blocks, 16, BLK), floats),
            pltpu.SMEM((slabs, -(-(1 + 2 * -(-slots // BLK)) // 8) * 8, BLK), floats),
            pltpu.SemaphoreType.DMA((slabs,)),
            pltpu.VMEM((total + 1, 16, BLK), floats),
            pltpu.VMEM((total + 1, 32, BLK), jnp.bfloat16),
            pltpu.VMEM((total, BLK, 32), jnp.bfloat16),
            pltpu.VMEM((total, 16, 2 * BLK), jnp.bfloat16),
            pltpu.VMEM((UNROLL, BLK, BLK), floats),
        ],
        compiler_params=pltpu.CompilerParams(vmem_limit_bytes=MAIN_VMEM),
    )(stiffness, inverse, *states, *fixeds)
    return tuple(out.reshape(positions.shape) for out in outs)


def solution(mesh):
    placed = (
        P("wrow", "wcol", None, "dom"),
        P("wrow", "wcol", None, "dom"),
        P("dom"),
        P(None, None, "dom"),
        P(),
        P("wrow", "wcol", None),
        P("dom"),
        P("dom"),
        P("dom", None),
        P("dom", None),
        P("wrow", "wcol"),
        P("wrow", "wcol"),
    )
    return jax.shard_map(
        per_device,
        mesh=mesh,
        in_specs=placed,
        out_specs=(P("wrow", "wcol", None, "dom"),) * 3,
        check_vma=False,
    )
```

```python
import functools
import math

import jax
import jax.numpy as jnp
from jax import lax
from jax.experimental import pallas as pl
from jax.experimental.pallas import tpu as pltpu
from jax.sharding import PartitionSpec as P

BLK = 128
STEPS = 3
PAIR_EPS = 0.015625
DT = 0.1
UNROLL = 16
PASS = 16
SMALL_VMEM = 4 << 20
MAIN_VMEM = 24 << 20
ROOT = math.sqrt(math.log2(math.e))


def rounded(x):
    return x.astype(jnp.bfloat16).astype(jnp.float32)


def lanes_from(source, low):
    return jnp.take_along_axis(source, low, axis=1, mode="promise_in_bounds")


def sub_row():
    return lax.broadcasted_iota(jnp.int32, (8, BLK), 0)


def is_fourth():
    row = sub_row()
    return (row == 3) | (row == 7)


def total4(value):
    value = value + pltpu.roll(value, 1, 0)
    return value + pltpu.roll(value, 2, 0)


def whole(value):
    return jnp.sum(jnp.sum(value, axis=0, keepdims=True), axis=1, keepdims=True)


def span(block):
    return pl.ds(pl.multiple_of(block * BLK, BLK), BLK)


def reordered(high, low, rows):
    found = []
    for b, group in enumerate(rows):
        here = high == b
        for k, row in enumerate(group):
            moved = lanes_from(jnp.broadcast_to(row, high.shape), low)
            if b:
                found[k] = jnp.where(here, moved, found[k])
            else:
                found.append(moved)
    return found


def state_kernel(blocks, centers, stiffness, pos, vel, mass, order, out):
    index = order[...]
    high, low = index // BLK, index % BLK
    refs = [(pos, 0), (pos, 1), (pos, 2), (mass, 0), (vel, 0), (vel, 1), (vel, 2)]
    rows = [
        [ref[k * blocks + b : k * blocks + b + 1, :] for ref, k in refs] for b in range(blocks)
    ]
    for k, value in enumerate(reordered(high, low, rows)):
        out[k * blocks : (k + 1) * blocks, :] = value
    lane = lax.broadcasted_iota(jnp.int32, (blocks, BLK), 1)
    aux = jnp.where(lane == 0, centers[0, 0], centers[0, 1])
    aux = jnp.where(lane == 2, stiffness[0], jnp.where(lane == 3, stiffness[1], aux))
    out[7 * blocks :, :] = aux


def weight_kernel(blocks, slots, count, cv, order, own, other, out):
    index = order[...]
    high, low = index // BLK, index % BLK
    rows = [
        [cv[pl.ds((c * blocks + b) * 2 + k, 1), :] for k in range(2) for c in range(3)]
        for b in range(blocks)
    ]
    out[3 * blocks : 4 * blocks, :] = jnp.zeros((blocks, BLK), jnp.float32)
    for k, value in enumerate(reordered(high, low, rows)):
        k = k + k // 3
        out[k * blocks : (k + 1) * blocks, :] = value
    out[7 * blocks :, :] = jnp.zeros((blocks, BLK), jnp.float32) + count[0].astype(jnp.float32)
    lines = -(-slots // BLK)
    for j in range(lines):
        wide = min(BLK, slots - j * BLK)
        at = slice(j * BLK, j * BLK + wide)
        mine = 7 * blocks + 1 + j
        out[mine : mine + 1, 0:wide] = own[0:1, at].astype(jnp.float32)
        out[mine + lines : mine + lines + 1, 0:wide] = other[0:1, at].astype(jnp.float32)


def inverse_kernel(blocks, order, inv):
    size = blocks * BLK
    listed = jnp.concatenate([order[b : b + 1, :] for b in range(blocks)], 1)
    high, low = listed // BLK, listed % BLK
    place = lax.broadcasted_iota(jnp.int32, (blocks, size), 1)
    hit_high = lax.broadcasted_iota(jnp.int32, (blocks, size), 0) == high
    hit_low = lax.broadcasted_iota(jnp.int32, (BLK, size), 0) == low
    left = jnp.concatenate(
        [
            jnp.where(hit_high, place // BLK, 0).astype(jnp.float32),
            jnp.where(hit_high, place % BLK, 0).astype(jnp.float32),
        ],
        0,
    ).astype(jnp.bfloat16)
    right = jnp.where(hit_low, 1.0, 0.0).astype(jnp.bfloat16)
    inv[...] = lax.dot_general(
        left, right, (((1,), (1,)), ((), ())), preferred_element_type=jnp.float32
    ).astype(jnp.int32)


def by_xor(slabs):
    return slabs & (slabs - 1) == 0


def slab_of(me, slot, slabs):
    return me ^ slot if by_xor(slabs) else (me + slot) % slabs


def slot_of(slab, me, slabs):
    return slab ^ me if by_xor(slabs) else (slab - me + slabs) % slabs


class Pairs:
    def __init__(self, total, bases, owners, others, acc, atab, ctab, htab, spread, parts):
        self.bases, self.owners, self.others = bases, owners, others
        self.acc, self.atab, self.ctab, self.htab = acc, atab, ctab, htab
        self.spread, self.parts = spread, parts
        atab[total] = jnp.zeros((32, BLK), jnp.bfloat16)
        parts[...] = jnp.zeros(parts.shape, jnp.float32)

    def tables(self, group):
        row, fourth = sub_row(), is_fourth()
        made = []
        for block, x in group:
            scaled = jnp.where(fourth, 0.0, x * ROOT)
            half = -0.5 * total4(scaled * scaled)
            base = jnp.where(fourth, half, scaled)
            s1 = rounded(base)
            rest = base - s1
            s2 = rounded(rest)
            s3 = rest - s2
            one = jnp.float32(1.0)
            zero = jnp.zeros_like(x)
            a0 = jnp.where(row == 7, s2, s1)
            a1 = jnp.where(row == 3, s3, jnp.where(row == 7, one, s2))
            a2 = jnp.where(row < 3, s1, jnp.where(fourth, one, s3))
            c0 = jnp.where(row < 3, s1, jnp.where(fourth, one, s2))
            c1 = jnp.where((row < 3) | (row == 7), s1, jnp.where(row == 3, one, s2))
            c2 = jnp.where((row < 3) | (row == 7), s3, jnp.where(row == 3, s2, s1))
            h0 = jnp.where(row == 3, one, jnp.where(row == 7, 0.0, jnp.where(row < 4, s1, s2)))
            h1 = jnp.where(row < 3, s3, 0.0)
            ours = jnp.concatenate([a0, a1, a2, zero], 0).astype(jnp.bfloat16)
            theirs = jnp.concatenate([c0, c1, c2, zero], 0).T.astype(jnp.bfloat16)
            heads = jnp.concatenate([h0, h1], 0).astype(jnp.bfloat16)
            made.append((block, ours, theirs, heads))
        for block, ours, theirs, heads in made:
            self.atab[block] = ours
            self.ctab[block] = theirs
            self.htab[block, :, :BLK] = heads
            self.htab[block, :, BLK:] = heads
            self.acc[block] = jnp.zeros((16, BLK), jnp.float32)

    def listed(self, refs, group):
        base = self.bases[0, group]
        line, lane = base // BLK, base % BLK
        return [[ref[line, lane + u] for u in range(UNROLL)] for ref in refs]

    def spreads(self, group):
        owners, others = self.listed([self.owners, self.others], group)
        return [
            jnp.dot(self.ctab[other], self.atab[own], preferred_element_type=jnp.float32)
            for own, other in zip(owners, others)
        ]

    def add(self, group):
        (owners,) = self.listed([self.owners], group)
        for u, own in enumerate(owners):
            self.acc[own] += self.parts[u]

    def run(self, limit):
        def some(group, _):
            later = self.spreads(group + 1)
            self.add(group - 1)
            new = []
            (others,) = self.listed([self.others], group)
            for u, other in enumerate(others):
                weight = jnp.exp2(jnp.minimum(self.spread[u], 0.0))
                upper = weight.astype(jnp.bfloat16)
                lower = (weight - upper.astype(jnp.float32)).astype(jnp.bfloat16)
                both = jnp.concatenate([upper, lower], 0)
                new.append(jnp.dot(self.htab[other], both, preferred_element_type=jnp.float32))
            for u in range(UNROLL):
                self.spread[u] = later[u]
            for u in range(UNROLL):
                self.parts[u] = new[u]
            return 0

        for u, value in enumerate(self.spreads(1)):
            self.spread[u] = value
        lax.fori_loop(1, limit + 1, some, 0)
        self.add(limit)
        self.parts[...] = jnp.zeros(self.parts.shape, jnp.float32)

    def force(self, got, x):
        fourth = is_fourth()
        moved = got[:8] + got[8:]
        moved = moved + pltpu.roll(moved, 4, 0)
        weight = total4(jnp.where(fourth, moved, 0.0))
        pair = (x * ROOT * weight - moved) * (PAIR_EPS / ROOT)
        return jnp.where(fourth, 0.0, pair)


def decode_kernel(slabs, blocks, slots, *refs):
    fixed_refs = refs[:slabs]
    bases, owners, others = refs[slabs:]
    me = lax.axis_index("dom").astype(jnp.int32)
    lines = -(-slots // BLK)
    total = slabs * blocks
    lane = lax.broadcasted_iota(jnp.int32, (1, BLK), 1)
    owners[...] = jnp.full(owners.shape, total, jnp.int32)
    others[...] = jnp.zeros(others.shape, jnp.int32)
    ends = []
    for slab in range(slabs):
        first = 7 * blocks
        live = fixed_refs[slab][first : first + 1, :].astype(jnp.int32)
        groups = (live + UNROLL - 1) // UNROLL
        ends.append(groups + ends[-1] if slab else groups)
        for line in range(lines):
            at = first + 1 + line
            inside = lane + line * BLK < live
            own = fixed_refs[slab][at : at + 1, :].astype(jnp.int32)
            q = fixed_refs[slab][at + lines : at + lines + 1, :].astype(jnp.int32)
            shift = jnp.where(q >= blocks, 1, 0) + jnp.where(q >= 2 * blocks, 1, 0)
            where = slot_of(slab_of(me, slab, slabs) + shift - 1, me, slabs)
            to = slab * lines + line
            owners[to : to + 1, :] = jnp.where(inside, own + slab * blocks, total)
            others[to : to + 1, :] = jnp.where(inside, q + (where - shift) * blocks, 0)
    for line in range(bases.shape[0]):
        group = lane + line * BLK - 1
        at = group * UNROLL
        for slab in range(1, slabs):
            there = slab * lines * BLK + (group - ends[slab - 1]) * UNROLL
            at = jnp.where(group >= ends[slab - 1], there, at)
        none = slabs * lines * BLK
        bases[line : line + 1, :] = jnp.where((group < 0) | (group >= ends[-1]), none, at)
    bases[0:1, :] = jnp.where(
        lane == BLK - 1, ends[-1], jnp.where(lane == BLK - 2, ends[0], bases[0:1, :])
    )


def steps_kernel(slabs, blocks, *refs):
    bases, owners, others, inv = refs[:4]
    state_refs = refs[4 : 4 + slabs]
    fixed_refs = refs[4 + slabs : 4 + 2 * slabs]
    x_out, v_out, f_out = refs[4 + 2 * slabs : 7 + 2 * slabs]
    xs, vs, ms, w0s, w1s, packed, *rest = refs[7 + 2 * slabs :]
    acc = rest[0]
    total = slabs * blocks
    row, fourth = sub_row(), is_fourth()
    aux = state_refs[0][7 * blocks : 7 * blocks + 1, :]
    centre = [aux[:, k : k + 1] for k in range(2)]
    stiff = [aux[:, k : k + 1] for k in range(2, 4)]
    zero = jnp.zeros((8, BLK), jnp.float32)

    def strided(ref, t):
        return ref[pl.ds(t, 8, stride=blocks), :]

    work = Pairs(total, bases, owners, others, *rest)

    sums = (zero, zero)
    for slab in range(slabs):

        def load(group, carry, slab=slab):
            done = []
            for u in range(PASS):
                t = group * PASS + u
                state = strided(state_refs[slab], t)
                m = jnp.broadcast_to(state[3:4], (8, BLK))
                state = jnp.where(fourth, 0.0, state)
                turned = pltpu.roll(state, 4, 0)
                x = jnp.where(row < 4, state, turned)
                v = jnp.where(row < 4, turned, state)
                w = jnp.where(fourth, 0.0, strided(fixed_refs[slab], t))
                turned = pltpu.roll(w, 4, 0)
                w0 = jnp.where(row < 4, w, turned)
                w1 = jnp.where(row < 4, turned, w)
                carry = carry[0] + w0 * x, carry[1] + w1 * x
                done.append((slab * blocks + t, x, v, m, w0, w1))
            for block, x, v, m, w0, w1 in done:
                xs[block] = x
                vs[block] = v
                ms[block] = m
                w0s[block] = w0
                w1s[block] = w1
            work.tables([(block, x) for block, x, *_ in done])
            return carry

        sums = lax.fori_loop(0, blocks // PASS, load, sums)

    def pulls(pair):
        return [stiff[k] * (0.5 * whole(pair[k]) - centre[k]) for k in range(2)]

    def step(number, sums):
        work.run(bases[0, BLK - 1])
        pull = pulls(sums)
        kick = jnp.where(number == 0, jnp.float32(0.5 * DT), jnp.float32(DT))

        def some(group, carry):
            moved = []
            for u in range(PASS):
                block = group * PASS + u
                x = xs[block]
                force = work.force(acc[block], x) - (pull[0] * w0s[block] + pull[1] * w1s[block])
                v = vs[block] + kick * ms[block] * force
                x = x + DT * v
                moved.append((block, x, v))
                carry = carry[0] + w0s[block] * x, carry[1] + w1s[block] * x
            for block, x, v in moved:
                xs[block] = x
                vs[block] = v
            work.tables([(block, x) for block, x, _ in moved])
            return carry

        return lax.fori_loop(0, total // PASS, some, (zero, zero))

    sums = lax.fori_loop(0, STEPS, step, sums)
    work.run(bases[0, BLK - 2])
    pull = pulls(sums)

    for block in range(blocks):
        x = xs[block]
        force = work.force(acc[block], x) - (pull[0] * w0s[block] + pull[1] * w1s[block])
        v = vs[block] + (0.5 * DT) * ms[block] * force
        packed[block, 0:8] = jnp.where(row < 4, x, v)
        packed[block, 8:16] = force
    rows = [
        [packed[b, k : k + 1, :] for k in (0, 1, 2, 4, 5, 6, 8, 9, 10)] for b in range(blocks)
    ]
    found = reordered(inv[:blocks, :], inv[blocks:, :], rows)
    for k, value in enumerate(found):
        out = (x_out, v_out, f_out)[k // 3]
        k = k % 3
        out[k * blocks : (k + 1) * blocks, :] = value


def swapped(value, axis, accept):
    pairs = [(i, i ^ 1) for i in range(lax.axis_size(axis))]
    return jnp.where(accept == 1, lax.ppermute(value, axis, pairs), value)


def round_dom(value):
    count = lax.axis_size("dom")
    return [value] + [
        lax.ppermute(value, "dom", [(slab_of(i, s, count), i) for i in range(count)])
        for s in range(1, count)
    ]


def per_device(
    positions,
    velocities,
    inv_mass,
    cv_weight,
    stiffness,
    centers,
    block_order,
    pair_count,
    pair_own,
    pair_other,
    accept_row,
    accept_col,
):
    size = block_order.shape[0]
    blocks = size // BLK
    slots = pair_own.shape[1]
    slabs = lax.axis_size("dom")
    total = slabs * blocks
    vmem = pl.BlockSpec(memory_space=pltpu.VMEM)
    smem = pl.BlockSpec(memory_space=pltpu.SMEM)
    floats = jnp.float32
    payload = jax.ShapeDtypeStruct((8 * blocks, BLK), floats)

    def lines(value):
        return value.reshape(-1, BLK)

    def small(flops):
        return dict(
            compiler_params=pltpu.CompilerParams(vmem_limit_bytes=SMALL_VMEM),
            cost_estimate=pl.CostEstimate(
                flops=flops, bytes_accessed=1 << 17, transcendentals=0
            ),
        )

    order = lines(block_order)
    state = pl.pallas_call(
        functools.partial(state_kernel, blocks),
        out_shape=payload,
        in_specs=[smem] * 2 + [vmem] * 4,
        out_specs=vmem,
    )(centers[0], stiffness, lines(positions), lines(velocities), lines(inv_mass), order)
    weights = cv_weight.reshape(2, 3, blocks, BLK).transpose(1, 2, 0, 3).reshape(-1, BLK)
    fixed = pl.pallas_call(
        functools.partial(weight_kernel, blocks, slots),
        out_shape=payload,
        in_specs=[smem] + [vmem] * 4,
        out_specs=vmem,
        **small(1 << 24),
    )(pair_count, weights, order, pair_own, pair_other)
    inverse = pl.pallas_call(
        functools.partial(inverse_kernel, blocks),
        out_shape=jax.ShapeDtypeStruct((2 * blocks, BLK), jnp.int32),
        in_specs=[vmem],
        out_specs=vmem,
        **small(1 << 24),
    )(order)

    state = swapped(state, "wrow", accept_row[0, 0])
    state = swapped(state, "wcol", accept_col[0, 0])
    fixeds = round_dom(fixed)
    states = round_dom(state)

    rows = -(-slots // BLK)
    assert slabs * -(-slots // UNROLL) + 4 <= BLK
    tables = [(1, BLK)] + [(slabs * rows + 1, BLK)] * 2
    listed = pl.pallas_call(
        functools.partial(decode_kernel, slabs, blocks, slots),
        out_shape=[jax.ShapeDtypeStruct(shape, jnp.int32) for shape in tables],
        in_specs=[vmem] * slabs,
        out_specs=[vmem] * 3,
        **small(1 << 24),
    )(*fixeds)

    part = pltpu.VMEM((total, 8, BLK), floats)
    outs = pl.pallas_call(
        functools.partial(steps_kernel, slabs, blocks),
        out_shape=[jax.ShapeDtypeStruct((3 * blocks, BLK), floats)] * 3,
        in_specs=[smem] * 3 + [vmem] * (1 + 2 * slabs),
        out_specs=[vmem] * 3,
        scratch_shapes=[part] * 5
        + [
            pltpu.VMEM((blocks, 16, BLK), floats),
            pltpu.VMEM((total + 1, 16, BLK), floats),
            pltpu.VMEM((total + 1, 32, BLK), jnp.bfloat16),
            pltpu.VMEM((total, BLK, 32), jnp.bfloat16),
            pltpu.VMEM((total, 16, 2 * BLK), jnp.bfloat16),
            pltpu.VMEM((UNROLL, BLK, BLK), floats),
            pltpu.VMEM((UNROLL, 16, BLK), floats),
        ],
        compiler_params=pltpu.CompilerParams(vmem_limit_bytes=MAIN_VMEM),
    )(*listed, inverse, *states, *fixeds)
    return tuple(out.reshape(positions.shape) for out in outs)


def solution(mesh):
    placed = (
        P("wrow", "wcol", None, "dom"),
        P("wrow", "wcol", None, "dom"),
        P("dom"),
        P(None, None, "dom"),
        P(),
        P("wrow", "wcol", None),
        P("dom"),
        P("dom"),
        P("dom", None),
        P("dom", None),
        P("wrow", "wcol"),
        P("wrow", "wcol"),
    )
    return jax.shard_map(
        per_device,
        mesh=mesh,
        in_specs=placed,
        out_specs=(P("wrow", "wcol", None, "dom"),) * 3,
        check_vma=False,
    )
```

```python
import functools
import math

import jax
import jax.numpy as jnp
from jax import lax
from jax.experimental import pallas as pl
from jax.experimental.pallas import tpu as pltpu
from jax.sharding import PartitionSpec as P

BLK = 128
STEPS = 3
PAIR_EPS = 0.015625
DT = 0.1
UNROLL = 16
PASS = 16
SMALL_VMEM = 4 << 20
MAIN_VMEM = 24 << 20
ROOT = math.sqrt(math.log2(math.e))


def rounded(x):
    return x.astype(jnp.bfloat16).astype(jnp.float32)


def lanes_from(source, low):
    return jnp.take_along_axis(source, low, axis=1, mode="promise_in_bounds")


def sub_row():
    return lax.broadcasted_iota(jnp.int32, (8, BLK), 0)


def is_fourth():
    row = sub_row()
    return (row == 3) | (row == 7)


def total4(value):
    value = value + pltpu.roll(value, 1, 0)
    return value + pltpu.roll(value, 2, 0)


def whole(value):
    return jnp.sum(jnp.sum(value, axis=0, keepdims=True), axis=1, keepdims=True)


def span(block):
    return pl.ds(pl.multiple_of(block * BLK, BLK), BLK)


def reordered(high, low, rows):
    found = []
    for b, group in enumerate(rows):
        here = high == b
        for k, row in enumerate(group):
            moved = lanes_from(jnp.broadcast_to(row, high.shape), low)
            if b:
                found[k] = jnp.where(here, moved, found[k])
            else:
                found.append(moved)
    return found


def state_kernel(blocks, centers, stiffness, pos, vel, mass, order, out):
    index = order[...]
    high, low = index // BLK, index % BLK
    refs = [(pos, 0), (pos, 1), (pos, 2), (mass, 0), (vel, 0), (vel, 1), (vel, 2)]
    rows = [
        [ref[k * blocks + b : k * blocks + b + 1, :] for ref, k in refs] for b in range(blocks)
    ]
    for k, value in enumerate(reordered(high, low, rows)):
        out[k * blocks : (k + 1) * blocks, :] = value
    lane = lax.broadcasted_iota(jnp.int32, (8, BLK), 1)
    aux = jnp.where(lane == 0, centers[0, 0], centers[0, 1])
    aux = jnp.where(lane == 2, stiffness[0], jnp.where(lane == 3, stiffness[1], aux))
    out[7 * blocks :, :] = aux


def weight_kernel(blocks, slots, count, cv, order, own, other, out):
    index = order[...]
    high, low = index // BLK, index % BLK
    rows = [
        [cv[pl.ds((c * blocks + b) * 2 + k, 1), :] for k in range(2) for c in range(3)]
        for b in range(blocks)
    ]
    for k, value in enumerate(reordered(high, low, rows)):
        out[k * blocks : (k + 1) * blocks, :] = value
    start = 6 * blocks
    out[start:, :] = jnp.zeros((out.shape[0] - start, BLK), jnp.float32) + count[0].astype(
        jnp.float32
    )
    lines = -(-slots // BLK)
    for j in range(lines):
        wide = min(BLK, slots - j * BLK)
        at = slice(j * BLK, j * BLK + wide)
        mine = start + 1 + j
        out[mine : mine + 1, 0:wide] = own[0:1, at].astype(jnp.float32)
        out[mine + lines : mine + lines + 1, 0:wide] = other[0:1, at].astype(jnp.float32)


def inverse_kernel(blocks, order, inv):
    size = blocks * BLK
    listed = jnp.concatenate([order[b : b + 1, :] for b in range(blocks)], 1)
    high, low = listed // BLK, listed % BLK
    place = lax.broadcasted_iota(jnp.int32, (blocks, size), 1)
    hit_high = lax.broadcasted_iota(jnp.int32, (blocks, size), 0) == high
    hit_low = lax.broadcasted_iota(jnp.int32, (BLK, size), 0) == low
    left = jnp.concatenate(
        [
            jnp.where(hit_high, place // BLK, 0).astype(jnp.float32),
            jnp.where(hit_high, place % BLK, 0).astype(jnp.float32),
        ],
        0,
    ).astype(jnp.bfloat16)
    right = jnp.where(hit_low, 1.0, 0.0).astype(jnp.bfloat16)
    inv[...] = lax.dot_general(
        left, right, (((1,), (1,)), ((), ())), preferred_element_type=jnp.float32
    ).astype(jnp.int32)


def by_xor(slabs):
    return slabs & (slabs - 1) == 0


def slab_of(me, slot, slabs):
    return me ^ slot if by_xor(slabs) else (me + slot) % slabs


def slot_of(slab, me, slabs):
    return slab ^ me if by_xor(slabs) else (slab - me + slabs) % slabs


class Pairs:
    def __init__(self, total, owners, others, acc, atab, ctab, htab, spread, parts):
        self.owners, self.others = owners, others
        self.acc, self.atab, self.ctab, self.htab = acc, atab, ctab, htab
        self.spread, self.parts = spread, parts
        atab[total] = jnp.zeros((32, BLK), jnp.bfloat16)
        parts[...] = jnp.zeros(parts.shape, jnp.float32)

    def tables(self, group):
        row, fourth = sub_row(), is_fourth()
        made = []
        for block, x in group:
            scaled = jnp.where(fourth, 0.0, x * ROOT)
            half = -0.5 * total4(scaled * scaled)
            base = jnp.where(fourth, half, scaled)
            s1 = rounded(base)
            rest = base - s1
            s2 = rounded(rest)
            s3 = rest - s2
            one = jnp.float32(1.0)
            zero = jnp.zeros_like(x)
            a0 = jnp.where(row == 7, s2, s1)
            a1 = jnp.where(row == 3, s3, jnp.where(row == 7, one, s2))
            a2 = jnp.where(row < 3, s1, jnp.where(fourth, one, s3))
            c0 = jnp.where(row < 3, s1, jnp.where(fourth, one, s2))
            c1 = jnp.where((row < 3) | (row == 7), s1, jnp.where(row == 3, one, s2))
            c2 = jnp.where((row < 3) | (row == 7), s3, jnp.where(row == 3, s2, s1))
            h0 = jnp.where(row == 3, one, jnp.where(row == 7, 0.0, jnp.where(row < 4, s1, s2)))
            h1 = jnp.where(row < 3, s3, 0.0)
            ours = jnp.concatenate([a0, a1, a2, zero], 0).astype(jnp.bfloat16)
            theirs = jnp.concatenate([c0, c1, c2, zero], 0).T.astype(jnp.bfloat16)
            heads = jnp.concatenate([h0, h1], 0).astype(jnp.bfloat16)
            made.append((block, ours, theirs, heads))
        for block, ours, theirs, heads in made:
            self.atab[block] = ours
            self.ctab[block] = theirs
            self.htab[block, :, :BLK] = heads
            self.htab[block, :, BLK:] = heads
            self.acc[block] = jnp.zeros((16, BLK), jnp.float32)

    def listed(self, refs, group):
        line, lane = group // (BLK // UNROLL), group % (BLK // UNROLL) * UNROLL
        return [[ref[line, lane + u] for u in range(UNROLL)] for ref in refs]

    def spreads(self, group):
        owners, others = self.listed([self.owners, self.others], group)
        return [
            jnp.dot(self.ctab[other], self.atab[own], preferred_element_type=jnp.float32)
            for own, other in zip(owners, others)
        ]

    def add(self, group):
        (owners,) = self.listed([self.owners], group)
        for u, own in enumerate(owners):
            self.acc[own] += self.parts[u]

    def run(self, limit):
        def some(group, _):
            later = self.spreads(group + 1)
            self.add(group - 1)
            new = []
            (others,) = self.listed([self.others], group)
            for u, other in enumerate(others):
                weight = jnp.exp2(jnp.minimum(self.spread[u], 0.0))
                upper = weight.astype(jnp.bfloat16)
                lower = (weight - upper.astype(jnp.float32)).astype(jnp.bfloat16)
                both = jnp.concatenate([upper, lower], 0)
                new.append(jnp.dot(self.htab[other], both, preferred_element_type=jnp.float32))
            for u in range(UNROLL):
                self.spread[u] = later[u]
            for u in range(UNROLL):
                self.parts[u] = new[u]
            return 0

        for u, value in enumerate(self.spreads(1)):
            self.spread[u] = value
        lax.fori_loop(1, limit + 1, some, 0)
        self.add(limit)
        self.parts[...] = jnp.zeros(self.parts.shape, jnp.float32)

    def force(self, got, x):
        fourth = is_fourth()
        moved = got[:8] + got[8:]
        moved = moved + pltpu.roll(moved, 4, 0)
        weight = total4(jnp.where(fourth, moved, 0.0))
        pair = (x * ROOT * weight - moved) * (PAIR_EPS / ROOT)
        return jnp.where(fourth, 0.0, pair)


def decode_kernel(slabs, blocks, slots, *refs):
    fixed_refs = refs[:slabs]
    counts, owners, others = refs[slabs:]
    me = lax.axis_index("dom").astype(jnp.int32)
    lines = -(-slots // BLK)
    total = slabs * blocks
    place = lax.broadcasted_iota(jnp.int32, owners.shape, 0) * BLK
    place = place + lax.broadcasted_iota(jnp.int32, owners.shape, 1) - UNROLL
    owner = jnp.full(owners.shape, total, jnp.int32)
    other = jnp.zeros(owners.shape, jnp.int32)
    start = jnp.zeros((1, BLK), jnp.int32)
    for slab in range(slabs):
        first = 6 * blocks
        live = fixed_refs[slab][first : first + 1, :].astype(jnp.int32)
        for line in range(lines):
            at = first + 1 + line
            own = fixed_refs[slab][at : at + 1, :].astype(jnp.int32)
            q = fixed_refs[slab][at + lines : at + lines + 1, :].astype(jnp.int32)
            shift = jnp.where(q >= blocks, 1, 0) + jnp.where(q >= 2 * blocks, 1, 0)
            where = slot_of(slab_of(me, slab, slabs) + shift - 1, me, slabs)
            rank = place - start - line * BLK
            inside = (rank >= 0) & (rank < BLK) & (rank < live - line * BLK)
            rank = jnp.clip(rank, 0, BLK - 1)
            own = jnp.broadcast_to(own + slab * blocks, owners.shape)
            q = jnp.broadcast_to(q + (where - shift) * blocks, owners.shape)
            owner = jnp.where(inside, lanes_from(own, rank), owner)
            other = jnp.where(inside, lanes_from(q, rank), other)
        start = start + live
        if slab == 0:
            mine = (live + UNROLL - 1) // UNROLL
    owners[...] = owner
    others[...] = other
    lane = lax.broadcasted_iota(jnp.int32, (1, BLK), 1)
    counts[...] = jnp.where(lane == 0, mine, (start + UNROLL - 1) // UNROLL)


def steps_kernel(slabs, blocks, *refs):
    counts, owners, others, inv = refs[:4]
    state_refs = refs[4 : 4 + slabs]
    fixed_refs = refs[4 + slabs : 4 + 2 * slabs]
    x_out, v_out, f_out = refs[4 + 2 * slabs : 7 + 2 * slabs]
    xs, vs, ms, w0s, w1s, packed, *rest = refs[7 + 2 * slabs :]
    acc = rest[0]
    total = slabs * blocks
    row, fourth = sub_row(), is_fourth()
    aux = state_refs[0][7 * blocks : 7 * blocks + 1, :]
    centre = [aux[:, k : k + 1] for k in range(2)]
    stiff = [aux[:, k : k + 1] for k in range(2, 4)]
    zero = jnp.zeros((8, BLK), jnp.float32)

    none = jnp.zeros((1, BLK), jnp.float32)

    def strided(ref, t, count):
        return ref[pl.ds(t, count, stride=blocks), :]

    work = Pairs(total, owners, others, *rest)

    sums = (zero, zero)
    for slab in range(slabs):

        def load(group, carry, slab=slab):
            done = []
            for u in range(PASS):
                t = group * PASS + u
                state = jnp.concatenate([strided(state_refs[slab], t, 7), none], 0)
                m = jnp.broadcast_to(state[3:4], (8, BLK))
                state = jnp.where(fourth, 0.0, state)
                turned = pltpu.roll(state, 4, 0)
                x = jnp.where(row < 4, state, turned)
                v = jnp.where(row < 4, turned, state)
                w = strided(fixed_refs[slab], t, 6)
                w = jnp.concatenate([w[:3], none, w[3:], none], 0)
                turned = pltpu.roll(w, 4, 0)
                w0 = jnp.where(row < 4, w, turned)
                w1 = jnp.where(row < 4, turned, w)
                carry = carry[0] + w0 * x, carry[1] + w1 * x
                done.append((slab * blocks + t, x, v, m, w0, w1))
            for block, x, v, m, w0, w1 in done:
                xs[block] = x
                vs[block] = v
                ms[block] = m
                w0s[block] = w0
                w1s[block] = w1
            work.tables([(block, x) for block, x, *_ in done])
            return carry

        sums = lax.fori_loop(0, blocks // PASS, load, sums)

    def pulls(pair):
        return [stiff[k] * (0.5 * whole(pair[k]) - centre[k]) for k in range(2)]

    def step(number, sums):
        work.run(counts[0, 1])
        pull = pulls(sums)
        kick = jnp.where(number == 0, jnp.float32(0.5 * DT), jnp.float32(DT))

        def some(group, carry):
            moved = []
            for u in range(PASS):
                block = group * PASS + u
                x = xs[block]
                force = work.force(acc[block], x) - (pull[0] * w0s[block] + pull[1] * w1s[block])
                v = vs[block] + kick * ms[block] * force
                x = x + DT * v
                moved.append((block, x, v))
                carry = carry[0] + w0s[block] * x, carry[1] + w1s[block] * x
            for block, x, v in moved:
                xs[block] = x
                vs[block] = v
            work.tables([(block, x) for block, x, _ in moved])
            return carry

        return lax.fori_loop(0, total // PASS, some, (zero, zero))

    sums = lax.fori_loop(0, STEPS, step, sums)
    work.run(counts[0, 0])
    pull = pulls(sums)

    for block in range(blocks):
        x = xs[block]
        force = work.force(acc[block], x) - (pull[0] * w0s[block] + pull[1] * w1s[block])
        v = vs[block] + (0.5 * DT) * ms[block] * force
        packed[block, 0:8] = jnp.where(row < 4, x, v)
        packed[block, 8:16] = force
    rows = [
        [packed[b, k : k + 1, :] for k in (0, 1, 2, 4, 5, 6, 8, 9, 10)] for b in range(blocks)
    ]
    found = reordered(inv[:blocks, :], inv[blocks:, :], rows)
    for k, value in enumerate(found):
        out = (x_out, v_out, f_out)[k // 3]
        k = k % 3
        out[k * blocks : (k + 1) * blocks, :] = value


def swapped(value, axis, accept):
    pairs = [(i, i ^ 1) for i in range(lax.axis_size(axis))]
    return jnp.where(accept == 1, lax.ppermute(value, axis, pairs), value)


def round_dom(value):
    count = lax.axis_size("dom")
    return [value] + [
        lax.ppermute(value, "dom", [(slab_of(i, s, count), i) for i in range(count)])
        for s in range(1, count)
    ]


def per_device(
    positions,
    velocities,
    inv_mass,
    cv_weight,
    stiffness,
    centers,
    block_order,
    pair_count,
    pair_own,
    pair_other,
    accept_row,
    accept_col,
):
    size = block_order.shape[0]
    blocks = size // BLK
    slots = pair_own.shape[1]
    slabs = lax.axis_size("dom")
    total = slabs * blocks
    vmem = pl.BlockSpec(memory_space=pltpu.VMEM)
    smem = pl.BlockSpec(memory_space=pltpu.SMEM)
    floats = jnp.float32
    tail = -(-(1 + 2 * -(-slots // BLK)) // 8) * 8

    def payload(count):
        return jax.ShapeDtypeStruct((count, BLK), floats)

    def lines(value):
        return value.reshape(-1, BLK)

    def small(flops):
        return dict(
            compiler_params=pltpu.CompilerParams(vmem_limit_bytes=SMALL_VMEM),
            cost_estimate=pl.CostEstimate(
                flops=flops, bytes_accessed=1 << 17, transcendentals=0
            ),
        )

    order = lines(block_order)
    state = pl.pallas_call(
        functools.partial(state_kernel, blocks),
        out_shape=payload(7 * blocks + 8),
        in_specs=[smem] * 2 + [vmem] * 4,
        out_specs=vmem,
    )(centers[0], stiffness, lines(positions), lines(velocities), lines(inv_mass), order)
    weights = cv_weight.reshape(2, 3, blocks, BLK).transpose(1, 2, 0, 3).reshape(-1, BLK)
    fixed = pl.pallas_call(
        functools.partial(weight_kernel, blocks, slots),
        out_shape=payload(6 * blocks + tail),
        in_specs=[smem] + [vmem] * 4,
        out_specs=vmem,
        **small(1 << 24),
    )(pair_count, weights, order, pair_own, pair_other)
    inverse = pl.pallas_call(
        functools.partial(inverse_kernel, blocks),
        out_shape=jax.ShapeDtypeStruct((2 * blocks, BLK), jnp.int32),
        in_specs=[vmem],
        out_specs=vmem,
        **small(1 << 24),
    )(order)

    state = swapped(state, "wrow", accept_row[0, 0])
    state = swapped(state, "wcol", accept_col[0, 0])
    fixeds = round_dom(fixed)
    states = round_dom(state)

    room = -(-(slabs * slots + 4 * UNROLL) // (8 * BLK)) * 8
    tables = [(1, BLK)] + [(room, BLK)] * 2
    listed = pl.pallas_call(
        functools.partial(decode_kernel, slabs, blocks, slots),
        out_shape=[jax.ShapeDtypeStruct(shape, jnp.int32) for shape in tables],
        in_specs=[vmem] * slabs,
        out_specs=[vmem] * 3,
        **small(1 << 24),
    )(*fixeds)

    part = pltpu.VMEM((total, 8, BLK), floats)
    outs = pl.pallas_call(
        functools.partial(steps_kernel, slabs, blocks),
        out_shape=[jax.ShapeDtypeStruct((3 * blocks, BLK), floats)] * 3,
        in_specs=[smem] * 3 + [vmem] * (1 + 2 * slabs),
        out_specs=[vmem] * 3,
        scratch_shapes=[part] * 5
        + [
            pltpu.VMEM((blocks, 16, BLK), floats),
            pltpu.VMEM((total + 1, 16, BLK), floats),
            pltpu.VMEM((total + 1, 32, BLK), jnp.bfloat16),
            pltpu.VMEM((total, BLK, 32), jnp.bfloat16),
            pltpu.VMEM((total, 16, 2 * BLK), jnp.bfloat16),
            pltpu.VMEM((UNROLL, BLK, BLK), floats),
            pltpu.VMEM((UNROLL, 16, BLK), floats),
        ],
        compiler_params=pltpu.CompilerParams(vmem_limit_bytes=MAIN_VMEM),
    )(*listed, inverse, *states, *fixeds)
    return tuple(out.reshape(positions.shape) for out in outs)


def solution(mesh):
    placed = (
        P("wrow", "wcol", None, "dom"),
        P("wrow", "wcol", None, "dom"),
        P("dom"),
        P(None, None, "dom"),
        P(),
        P("wrow", "wcol", None),
        P("dom"),
        P("dom"),
        P("dom", None),
        P("dom", None),
        P("wrow", "wcol"),
        P("wrow", "wcol"),
    )
    return jax.shard_map(
        per_device,
        mesh=mesh,
        in_specs=placed,
        out_specs=(P("wrow", "wcol", None, "dom"),) * 3,
        check_vma=False,
    )
```

```python
import functools
import math

import jax
import jax.numpy as jnp
from jax import lax
from jax.experimental import pallas as pl
from jax.experimental.pallas import tpu as pltpu
from jax.sharding import PartitionSpec as P

BLK = 128
STEPS = 3
PAIR_EPS = 0.015625
DT = 0.1
UNROLL = 16
PASS = 16
WIDE = 32
SMALL_VMEM = 4 << 20
MAIN_VMEM = 24 << 20
ROOT = math.sqrt(math.log2(math.e))


def rounded(x):
    return x.astype(jnp.bfloat16).astype(jnp.float32)


def lanes_from(source, low):
    return jnp.take_along_axis(source, low, axis=1, mode="promise_in_bounds")


def sub_row():
    return lax.broadcasted_iota(jnp.int32, (8, BLK), 0)


def is_fourth():
    row = sub_row()
    return (row == 3) | (row == 7)


def total4(value):
    value = value + pltpu.roll(value, 1, 0)
    return value + pltpu.roll(value, 2, 0)


def whole(value):
    return jnp.sum(jnp.sum(value, axis=0, keepdims=True), axis=1, keepdims=True)


def span(block):
    return pl.ds(pl.multiple_of(block * BLK, BLK), BLK)


def reordered(high, low, rows):
    found = []
    for b, group in enumerate(rows):
        here = high == b
        for k, row in enumerate(group):
            moved = lanes_from(jnp.broadcast_to(row, high.shape), low)
            if b:
                found[k] = jnp.where(here, moved, found[k])
            else:
                found.append(moved)
    return found


def state_kernel(blocks, centers, stiffness, pos, vel, mass, order, out):
    index = order[...]
    high, low = index // BLK, index % BLK
    refs = [(pos, 0), (pos, 1), (pos, 2), (mass, 0), (vel, 0), (vel, 1), (vel, 2)]
    rows = [
        [ref[k * blocks + b : k * blocks + b + 1, :] for ref, k in refs] for b in range(blocks)
    ]
    for k, value in enumerate(reordered(high, low, rows)):
        out[k * blocks : (k + 1) * blocks, :] = value
    lane = lax.broadcasted_iota(jnp.int32, (8, BLK), 1)
    aux = jnp.where(lane == 0, centers[0, 0], centers[0, 1])
    aux = jnp.where(lane == 2, stiffness[0], jnp.where(lane == 3, stiffness[1], aux))
    out[7 * blocks :, :] = aux


def weight_kernel(blocks, slots, count, cv, order, own, other, out, half):
    index = order[...]
    high, low = index // BLK, index % BLK
    rows = [
        [cv[pl.ds((c * blocks + b) * 2 + k, 1), :] for k in range(2) for c in range(3)]
        for b in range(blocks)
    ]
    odd = lax.rem(lax.axis_index("wrow"), 2) == 1
    found = reordered(high, low, rows)
    for k, value in enumerate(found):
        out[k * blocks : (k + 1) * blocks, :] = value
    for k in range(3):
        half[k * blocks : (k + 1) * blocks, :] = jnp.where(odd, found[k + 3], found[k])
    start = 6 * blocks
    out[start:, :] = jnp.zeros((out.shape[0] - start, BLK), jnp.float32) + count[0].astype(
        jnp.float32
    )
    lines = -(-slots // BLK)
    for j in range(lines):
        wide = min(BLK, slots - j * BLK)
        at = slice(j * BLK, j * BLK + wide)
        mine = start + 1 + j
        out[mine : mine + 1, 0:wide] = own[0:1, at].astype(jnp.float32)
        out[mine + lines : mine + lines + 1, 0:wide] = other[0:1, at].astype(jnp.float32)
    half[3 * blocks :, :] = out[start:, :]


def inverse_kernel(blocks, order, inv):
    size = blocks * BLK
    listed = jnp.concatenate([order[b : b + 1, :] for b in range(blocks)], 1)
    high, low = listed // BLK, listed % BLK
    place = lax.broadcasted_iota(jnp.int32, (blocks, size), 1)
    hit_high = lax.broadcasted_iota(jnp.int32, (blocks, size), 0) == high
    hit_low = lax.broadcasted_iota(jnp.int32, (BLK, size), 0) == low
    left = jnp.concatenate(
        [
            jnp.where(hit_high, place // BLK, 0).astype(jnp.float32),
            jnp.where(hit_high, place % BLK, 0).astype(jnp.float32),
        ],
        0,
    ).astype(jnp.bfloat16)
    right = jnp.where(hit_low, 1.0, 0.0).astype(jnp.bfloat16)
    inv[...] = lax.dot_general(
        left, right, (((1,), (1,)), ((), ())), preferred_element_type=jnp.float32
    ).astype(jnp.int32)


def by_xor(slabs):
    return slabs & (slabs - 1) == 0


def slab_of(me, slot, slabs):
    return me ^ slot if by_xor(slabs) else (me + slot) % slabs


def slot_of(slab, me, slabs):
    return slab ^ me if by_xor(slabs) else (slab - me + slabs) % slabs


class Pairs:
    def __init__(self, total, owners, others, acc, atab, ctab, htab, spread, parts):
        self.owners, self.others = owners, others
        self.acc, self.atab, self.ctab, self.htab = acc, atab, ctab, htab
        self.spread, self.parts = spread, parts
        atab[total] = jnp.zeros((32, BLK), jnp.bfloat16)
        parts[...] = jnp.zeros(parts.shape, jnp.float32)

    def tables(self, group):
        row, fourth = sub_row(), is_fourth()
        made = []
        for block, x in group:
            scaled = jnp.where(fourth, 0.0, x * ROOT)
            half = -0.5 * total4(scaled * scaled)
            base = jnp.where(fourth, half, scaled)
            s1 = rounded(base)
            rest = base - s1
            s2 = rounded(rest)
            s3 = rest - s2
            one = jnp.float32(1.0)
            zero = jnp.zeros_like(x)
            a0 = jnp.where(row == 7, s2, s1)
            a1 = jnp.where(row == 3, s3, jnp.where(row == 7, one, s2))
            a2 = jnp.where(row < 3, s1, jnp.where(fourth, one, s3))
            c0 = jnp.where(row < 3, s1, jnp.where(fourth, one, s2))
            c1 = jnp.where((row < 3) | (row == 7), s1, jnp.where(row == 3, one, s2))
            c2 = jnp.where((row < 3) | (row == 7), s3, jnp.where(row == 3, s2, s1))
            h0 = jnp.where(row == 3, one, jnp.where(row == 7, 0.0, jnp.where(row < 4, s1, s2)))
            h1 = jnp.where(row < 3, s3, 0.0)
            ours = jnp.concatenate([a0, a1, a2, zero], 0).astype(jnp.bfloat16)
            theirs = jnp.concatenate([c0, c1, c2, zero], 0).T.astype(jnp.bfloat16)
            heads = jnp.concatenate([h0, h1], 0).astype(jnp.bfloat16)
            made.append((block, ours, theirs, heads))
        for block, ours, theirs, heads in made:
            self.atab[block] = ours
            self.ctab[block] = theirs
            self.htab[block, :, :BLK] = heads
            self.htab[block, :, BLK:] = heads
            self.acc[block] = jnp.zeros((16, BLK), jnp.float32)

    def listed(self, refs, group):
        line, lane = group // (BLK // UNROLL), group % (BLK // UNROLL) * UNROLL
        return [[ref[line, lane + u] for u in range(UNROLL)] for ref in refs]

    def spreads(self, group):
        owners, others = self.listed([self.owners, self.others], group)
        return [
            jnp.dot(self.ctab[other], self.atab[own], preferred_element_type=jnp.float32)
            for own, other in zip(owners, others)
        ]

    def add(self, group):
        (owners,) = self.listed([self.owners], group)
        for u, own in enumerate(owners):
            self.acc[own] += self.parts[u]

    def run(self, limit):
        def some(group, _):
            later = self.spreads(group + 1)
            self.add(group - 1)
            new = []
            (others,) = self.listed([self.others], group)
            for u, other in enumerate(others):
                weight = jnp.exp2(jnp.minimum(self.spread[u], 0.0))
                upper = weight.astype(jnp.bfloat16)
                lower = (weight - upper.astype(jnp.float32)).astype(jnp.bfloat16)
                both = jnp.concatenate([upper, lower], 0)
                new.append(jnp.dot(self.htab[other], both, preferred_element_type=jnp.float32))
            for u in range(UNROLL):
                self.spread[u] = later[u]
            for u in range(UNROLL):
                self.parts[u] = new[u]
            return 0

        for u, value in enumerate(self.spreads(1)):
            self.spread[u] = value
        lax.fori_loop(1, limit + 1, some, 0)
        self.add(limit)
        self.parts[...] = jnp.zeros(self.parts.shape, jnp.float32)

    def force(self, got, x):
        fourth = is_fourth()
        moved = got[:8] + got[8:]
        moved = moved + pltpu.roll(moved, 4, 0)
        weight = total4(jnp.where(fourth, moved, 0.0))
        pair = (x * ROOT * weight - moved) * (PAIR_EPS / ROOT)
        return jnp.where(fourth, 0.0, pair)


def decode_kernel(slabs, blocks, slots, *refs):
    fixed_refs = refs[:slabs]
    counts, owners, others = refs[slabs:]
    me = lax.axis_index("dom").astype(jnp.int32)
    lines = -(-slots // BLK)
    total = slabs * blocks
    place = lax.broadcasted_iota(jnp.int32, owners.shape, 0) * BLK
    place = place + lax.broadcasted_iota(jnp.int32, owners.shape, 1) - UNROLL
    owner = jnp.full(owners.shape, total, jnp.int32)
    other = jnp.zeros(owners.shape, jnp.int32)
    start = jnp.zeros((1, BLK), jnp.int32)
    for slab in range(slabs):
        first = (3 if slab else 6) * blocks
        live = fixed_refs[slab][first : first + 1, :].astype(jnp.int32)
        for line in range(lines):
            at = first + 1 + line
            own = fixed_refs[slab][at : at + 1, :].astype(jnp.int32)
            q = fixed_refs[slab][at + lines : at + lines + 1, :].astype(jnp.int32)
            shift = jnp.where(q >= blocks, 1, 0) + jnp.where(q >= 2 * blocks, 1, 0)
            where = slot_of(slab_of(me, slab, slabs) + shift - 1, me, slabs)
            rank = place - start - line * BLK
            inside = (rank >= 0) & (rank < BLK) & (rank < live - line * BLK)
            rank = jnp.clip(rank, 0, BLK - 1)
            own = jnp.broadcast_to(own + slab * blocks, owners.shape)
            q = jnp.broadcast_to(q + (where - shift) * blocks, owners.shape)
            owner = jnp.where(inside, lanes_from(own, rank), owner)
            other = jnp.where(inside, lanes_from(q, rank), other)
        start = start + live
        if slab == 0:
            mine = (live + UNROLL - 1) // UNROLL
    owners[...] = owner
    others[...] = other
    lane = lax.broadcasted_iota(jnp.int32, (1, BLK), 1)
    counts[...] = jnp.where(lane == 0, mine, (start + UNROLL - 1) // UNROLL)


def steps_kernel(slabs, blocks, *refs):
    counts, owners, others, inv = refs[:4]
    state_refs = refs[4 : 4 + slabs]
    fixed_refs = refs[4 + slabs : 4 + 2 * slabs]
    twin_refs = [None, *refs[4 + 2 * slabs : 3 + 3 * slabs]]
    x_out, v_out, f_out = refs[3 + 3 * slabs : 6 + 3 * slabs]
    xs, vs, ms, w0s, w1s, packed, *rest = refs[6 + 3 * slabs :]
    odd = lax.rem(lax.axis_index("wrow"), 2) == 1
    acc = rest[0]
    total = slabs * blocks
    row, fourth = sub_row(), is_fourth()
    aux = state_refs[0][7 * blocks : 7 * blocks + 1, :]
    centre = [aux[:, k : k + 1] for k in range(2)]
    stiff = [aux[:, k : k + 1] for k in range(2, 4)]
    zero = jnp.zeros((8, BLK), jnp.float32)

    none = jnp.zeros((1, BLK), jnp.float32)

    def strided(ref, t, count):
        return ref[pl.ds(t, count, stride=blocks), :]

    work = Pairs(total, owners, others, *rest)

    sums = (zero, zero)
    for slab in range(slabs):

        def load(group, carry, slab=slab):
            done = []
            for u in range(PASS):
                t = group * PASS + u
                state = jnp.concatenate([strided(state_refs[slab], t, 7), none], 0)
                m = jnp.broadcast_to(state[3:4], (8, BLK))
                state = jnp.where(fourth, 0.0, state)
                turned = pltpu.roll(state, 4, 0)
                x = jnp.where(row < 4, state, turned)
                v = jnp.where(row < 4, turned, state)
                if slab:
                    mine = strided(fixed_refs[slab], t, 3)
                    twin = strided(twin_refs[slab], t, 3)
                else:
                    w = strided(fixed_refs[slab], t, 6)
                    mine, twin = w[:3], w[3:]
                w = jnp.concatenate([mine, none, twin, none], 0)
                turned = pltpu.roll(w, 4, 0)
                w0 = jnp.where(row < 4, w, turned)
                w1 = jnp.where(row < 4, turned, w)
                if slab:
                    w0, w1 = jnp.where(odd, w1, w0), jnp.where(odd, w0, w1)
                carry = carry[0] + w0 * x, carry[1] + w1 * x
                done.append((slab * blocks + t, x, v, m, w0, w1))
            for block, x, v, m, w0, w1 in done:
                xs[block] = x
                vs[block] = v
                ms[block] = m
                w0s[block] = w0
                w1s[block] = w1
            work.tables([(block, x) for block, x, *_ in done])
            return carry

        sums = lax.fori_loop(0, blocks // PASS, load, sums)

    def pulls(pair):
        return [stiff[k] * (0.5 * whole(pair[k]) - centre[k]) for k in range(2)]

    def step(number, sums):
        work.run(counts[0, 1])
        pull = pulls(sums)
        kick = jnp.where(number == 0, jnp.float32(0.5 * DT), jnp.float32(DT))

        def some(group, carry):
            moved = []
            for u in range(WIDE):
                block = group * WIDE + u
                x = xs[block]
                force = work.force(acc[block], x) - (pull[0] * w0s[block] + pull[1] * w1s[block])
                v = vs[block] + kick * ms[block] * force
                x = x + DT * v
                moved.append((block, x, v))
                carry = carry[0] + w0s[block] * x, carry[1] + w1s[block] * x
            for block, x, v in moved:
                xs[block] = x
                vs[block] = v
            work.tables([(block, x) for block, x, _ in moved])
            return carry

        return lax.fori_loop(0, total // WIDE, some, (zero, zero))

    sums = lax.fori_loop(0, STEPS, step, sums)
    work.run(counts[0, 0])
    pull = pulls(sums)

    for block in range(blocks):
        x = xs[block]
        force = work.force(acc[block], x) - (pull[0] * w0s[block] + pull[1] * w1s[block])
        v = vs[block] + (0.5 * DT) * ms[block] * force
        packed[block, 0:8] = jnp.where(row < 4, x, v)
        packed[block, 8:16] = force
    rows = [
        [packed[b, k : k + 1, :] for k in (0, 1, 2, 4, 5, 6, 8, 9, 10)] for b in range(blocks)
    ]
    found = reordered(inv[:blocks, :], inv[blocks:, :], rows)
    for k, value in enumerate(found):
        out = (x_out, v_out, f_out)[k // 3]
        k = k % 3
        out[k * blocks : (k + 1) * blocks, :] = value


def swapped(value, axis, accept):
    pairs = [(i, i ^ 1) for i in range(lax.axis_size(axis))]
    return jnp.where(accept == 1, lax.ppermute(value, axis, pairs), value)


def round_dom(value):
    count = lax.axis_size("dom")
    return [value] + [
        lax.ppermute(value, "dom", [(slab_of(i, s, count), i) for i in range(count)])
        for s in range(1, count)
    ]


def per_device(
    positions,
    velocities,
    inv_mass,
    cv_weight,
    stiffness,
    centers,
    block_order,
    pair_count,
    pair_own,
    pair_other,
    accept_row,
    accept_col,
):
    size = block_order.shape[0]
    blocks = size // BLK
    slots = pair_own.shape[1]
    slabs = lax.axis_size("dom")
    total = slabs * blocks
    vmem = pl.BlockSpec(memory_space=pltpu.VMEM)
    smem = pl.BlockSpec(memory_space=pltpu.SMEM)
    floats = jnp.float32
    tail = -(-(1 + 2 * -(-slots // BLK)) // 8) * 8

    def payload(count):
        return jax.ShapeDtypeStruct((count, BLK), floats)

    def lines(value):
        return value.reshape(-1, BLK)

    def small(flops):
        return dict(
            compiler_params=pltpu.CompilerParams(vmem_limit_bytes=SMALL_VMEM),
            cost_estimate=pl.CostEstimate(
                flops=flops, bytes_accessed=1 << 17, transcendentals=0
            ),
        )

    order = lines(block_order)
    state = pl.pallas_call(
        functools.partial(state_kernel, blocks),
        out_shape=payload(7 * blocks + 8),
        in_specs=[smem] * 2 + [vmem] * 4,
        out_specs=vmem,
    )(centers[0], stiffness, lines(positions), lines(velocities), lines(inv_mass), order)
    weights = cv_weight.reshape(2, 3, blocks, BLK).transpose(1, 2, 0, 3).reshape(-1, BLK)
    fixed, half = pl.pallas_call(
        functools.partial(weight_kernel, blocks, slots),
        out_shape=[payload(6 * blocks + tail), payload(3 * blocks + tail)],
        in_specs=[smem] + [vmem] * 4,
        out_specs=[vmem] * 2,
        **small(1 << 24),
    )(pair_count, weights, order, pair_own, pair_other)
    inverse = pl.pallas_call(
        functools.partial(inverse_kernel, blocks),
        out_shape=jax.ShapeDtypeStruct((2 * blocks, BLK), jnp.int32),
        in_specs=[vmem],
        out_specs=vmem,
        **small(1 << 24),
    )(order)

    state = swapped(state, "wrow", accept_row[0, 0])
    state = swapped(state, "wcol", accept_col[0, 0])
    fixeds = [fixed] + round_dom(half)[1:]
    states = round_dom(state)
    flips = [(i, i ^ 1) for i in range(lax.axis_size("wrow"))]
    twins = [lax.ppermute(value, "wrow", flips) for value in fixeds[1:]]

    room = -(-(slabs * slots + 4 * UNROLL) // (8 * BLK)) * 8
    tables = [(1, BLK)] + [(room, BLK)] * 2
    listed = pl.pallas_call(
        functools.partial(decode_kernel, slabs, blocks, slots),
        out_shape=[jax.ShapeDtypeStruct(shape, jnp.int32) for shape in tables],
        in_specs=[vmem] * slabs,
        out_specs=[vmem] * 3,
        **small(1 << 24),
    )(*fixeds)

    part = pltpu.VMEM((total, 8, BLK), floats)
    outs = pl.pallas_call(
        functools.partial(steps_kernel, slabs, blocks),
        out_shape=[jax.ShapeDtypeStruct((3 * blocks, BLK), floats)] * 3,
        in_specs=[smem] * 3 + [vmem] * (3 * slabs),
        out_specs=[vmem] * 3,
        scratch_shapes=[part] * 5
        + [
            pltpu.VMEM((blocks, 16, BLK), floats),
            pltpu.VMEM((total + 1, 16, BLK), floats),
            pltpu.VMEM((total + 1, 32, BLK), jnp.bfloat16),
            pltpu.VMEM((total, BLK, 32), jnp.bfloat16),
            pltpu.VMEM((total, 16, 2 * BLK), jnp.bfloat16),
            pltpu.VMEM((UNROLL, BLK, BLK), floats),
            pltpu.VMEM((UNROLL, 16, BLK), floats),
        ],
        compiler_params=pltpu.CompilerParams(vmem_limit_bytes=MAIN_VMEM),
    )(*listed, inverse, *states, *fixeds, *twins)
    return tuple(out.reshape(positions.shape) for out in outs)


def solution(mesh):
    placed = (
        P("wrow", "wcol", None, "dom"),
        P("wrow", "wcol", None, "dom"),
        P("dom"),
        P(None, None, "dom"),
        P(),
        P("wrow", "wcol", None),
        P("dom"),
        P("dom"),
        P("dom", None),
        P("dom", None),
        P("wrow", "wcol"),
        P("wrow", "wcol"),
    )
    return jax.shard_map(
        per_device,
        mesh=mesh,
        in_specs=placed,
        out_specs=(P("wrow", "wcol", None, "dom"),) * 3,
        check_vma=False,
    )
```

```python
import functools
import math

import jax
import jax.numpy as jnp
from jax import lax
from jax.experimental import pallas as pl
from jax.experimental.pallas import tpu as pltpu
from jax.sharding import PartitionSpec as P

BLK = 128
STEPS = 3
PAIR_EPS = 0.015625
DT = 0.1
UNROLL = 16
PASS = 16
WIDE = 64
SMALL_VMEM = 4 << 20
MAIN_VMEM = 24 << 20
ROOT = math.sqrt(math.log2(math.e))


def rounded(x):
    return x.astype(jnp.bfloat16).astype(jnp.float32)


def lanes_from(source, low):
    return jnp.take_along_axis(source, low, axis=1, mode="promise_in_bounds")


def sub_row():
    return lax.broadcasted_iota(jnp.int32, (8, BLK), 0)


def is_fourth():
    row = sub_row()
    return (row == 3) | (row == 7)


def total4(value):
    value = value + pltpu.roll(value, 1, 0)
    return value + pltpu.roll(value, 2, 0)


def whole(value):
    return jnp.sum(jnp.sum(value, axis=0, keepdims=True), axis=1, keepdims=True)


def span(block):
    return pl.ds(pl.multiple_of(block * BLK, BLK), BLK)


def reordered(high, low, rows):
    found = []
    for b, group in enumerate(rows):
        here = high == b
        for k, row in enumerate(group):
            moved = lanes_from(jnp.broadcast_to(row, high.shape), low)
            if b:
                found[k] = jnp.where(here, moved, found[k])
            else:
                found.append(moved)
    return found


def state_kernel(blocks, centers, stiffness, pos, vel, mass, order, out):
    index = order[...]
    high, low = index // BLK, index % BLK
    refs = [(pos, 0), (pos, 1), (pos, 2), (mass, 0), (vel, 0), (vel, 1), (vel, 2)]
    rows = [
        [ref[k * blocks + b : k * blocks + b + 1, :] for ref, k in refs] for b in range(blocks)
    ]
    for k, value in enumerate(reordered(high, low, rows)):
        out[k * blocks : (k + 1) * blocks, :] = value
    lane = lax.broadcasted_iota(jnp.int32, (8, BLK), 1)
    aux = jnp.where(lane == 0, centers[0, 0], centers[0, 1])
    aux = jnp.where(lane == 2, stiffness[0], jnp.where(lane == 3, stiffness[1], aux))
    out[7 * blocks :, :] = aux


def weight_kernel(blocks, slots, count, cv, order, own, other, out, half):
    index = order[...]
    high, low = index // BLK, index % BLK
    rows = [
        [cv[pl.ds((c * blocks + b) * 2 + k, 1), :] for k in range(2) for c in range(3)]
        for b in range(blocks)
    ]
    odd = lax.rem(lax.axis_index("wrow"), 2) == 1
    found = reordered(high, low, rows)
    for k, value in enumerate(found):
        out[k * blocks : (k + 1) * blocks, :] = value
    for k in range(3):
        half[k * blocks : (k + 1) * blocks, :] = jnp.where(odd, found[k + 3], found[k])
    start = 6 * blocks
    out[start:, :] = jnp.zeros((out.shape[0] - start, BLK), jnp.float32) + count[0].astype(
        jnp.float32
    )
    lines = -(-slots // BLK)
    for j in range(lines):
        wide = min(BLK, slots - j * BLK)
        at = slice(j * BLK, j * BLK + wide)
        mine = start + 1 + j
        out[mine : mine + 1, 0:wide] = own[0:1, at].astype(jnp.float32)
        out[mine + lines : mine + lines + 1, 0:wide] = other[0:1, at].astype(jnp.float32)
    half[3 * blocks :, :] = out[start:, :]


def inverse_kernel(blocks, order, inv):
    size = blocks * BLK
    listed = jnp.concatenate([order[b : b + 1, :] for b in range(blocks)], 1)
    high, low = listed // BLK, listed % BLK
    place = lax.broadcasted_iota(jnp.int32, (blocks, size), 1)
    hit_high = lax.broadcasted_iota(jnp.int32, (blocks, size), 0) == high
    hit_low = lax.broadcasted_iota(jnp.int32, (BLK, size), 0) == low
    left = jnp.concatenate(
        [
            jnp.where(hit_high, place // BLK, 0).astype(jnp.float32),
            jnp.where(hit_high, place % BLK, 0).astype(jnp.float32),
        ],
        0,
    ).astype(jnp.bfloat16)
    right = jnp.where(hit_low, 1.0, 0.0).astype(jnp.bfloat16)
    inv[...] = lax.dot_general(
        left, right, (((1,), (1,)), ((), ())), preferred_element_type=jnp.float32
    ).astype(jnp.int32)


def by_xor(slabs):
    return slabs & (slabs - 1) == 0


def slab_of(me, slot, slabs):
    return me ^ slot if by_xor(slabs) else (me + slot) % slabs


def slot_of(slab, me, slabs):
    return slab ^ me if by_xor(slabs) else (slab - me + slabs) % slabs


class Pairs:
    def __init__(self, total, owners, others, acc, atab, ctab, htab, spread, parts):
        self.owners, self.others = owners, others
        self.acc, self.atab, self.ctab, self.htab = acc, atab, ctab, htab
        self.spread, self.parts = spread, parts
        atab[total] = jnp.zeros((32, BLK), jnp.bfloat16)
        parts[...] = jnp.zeros(parts.shape, jnp.float32)

    def tables(self, group):
        row, fourth = sub_row(), is_fourth()
        made = []
        for block, x in group:
            scaled = jnp.where(fourth, 0.0, x * ROOT)
            half = -0.5 * total4(scaled * scaled)
            base = jnp.where(fourth, half, scaled)
            s1 = rounded(base)
            rest = base - s1
            s2 = rounded(rest)
            s3 = rest - s2
            one = jnp.float32(1.0)
            zero = jnp.zeros_like(x)
            a0 = jnp.where(row == 7, s2, s1)
            a1 = jnp.where(row == 3, s3, jnp.where(row == 7, one, s2))
            a2 = jnp.where(row < 3, s1, jnp.where(fourth, one, s3))
            c0 = jnp.where(row < 3, s1, jnp.where(fourth, one, s2))
            c1 = jnp.where((row < 3) | (row == 7), s1, jnp.where(row == 3, one, s2))
            c2 = jnp.where((row < 3) | (row == 7), s3, jnp.where(row == 3, s2, s1))
            h0 = jnp.where(row == 3, one, jnp.where(row == 7, 0.0, jnp.where(row < 4, s1, s2)))
            h1 = jnp.where(row < 3, s3, 0.0)
            ours = jnp.concatenate([a0, a1, a2, zero], 0).astype(jnp.bfloat16)
            theirs = jnp.concatenate([c0, c1, c2, zero], 0).T.astype(jnp.bfloat16)
            heads = jnp.concatenate([h0, h1], 0).astype(jnp.bfloat16)
            made.append((block, ours, theirs, heads))
        for block, ours, theirs, heads in made:
            self.atab[block] = ours
            self.ctab[block] = theirs
            self.htab[block, :, :BLK] = heads
            self.htab[block, :, BLK:] = heads
            self.acc[block] = jnp.zeros((16, BLK), jnp.float32)

    def listed(self, refs, group):
        line, lane = group // (BLK // UNROLL), group % (BLK // UNROLL) * UNROLL
        return [[ref[line, lane + u] for u in range(UNROLL)] for ref in refs]

    def spreads(self, group):
        owners, others = self.listed([self.owners, self.others], group)
        return [
            jnp.dot(self.ctab[other], self.atab[own], preferred_element_type=jnp.float32)
            for own, other in zip(owners, others)
        ]

    def add(self, group):
        (owners,) = self.listed([self.owners], group)
        for u, own in enumerate(owners):
            self.acc[own] += self.parts[u]

    def run(self, limit):
        def some(group, _):
            later = self.spreads(group + 1)
            self.add(group - 1)
            new = []
            (others,) = self.listed([self.others], group)
            for u, other in enumerate(others):
                weight = jnp.exp2(jnp.minimum(self.spread[u], 0.0))
                upper = weight.astype(jnp.bfloat16)
                lower = (weight - upper.astype(jnp.float32)).astype(jnp.bfloat16)
                both = jnp.concatenate([upper, lower], 0)
                new.append(jnp.dot(self.htab[other], both, preferred_element_type=jnp.float32))
            for u in range(UNROLL):
                self.spread[u] = later[u]
            for u in range(UNROLL):
                self.parts[u] = new[u]
            return 0

        for u, value in enumerate(self.spreads(1)):
            self.spread[u] = value
        lax.fori_loop(1, limit + 1, some, 0)
        self.add(limit)
        self.parts[...] = jnp.zeros(self.parts.shape, jnp.float32)

    def force(self, got, x):
        fourth = is_fourth()
        moved = got[:8] + got[8:]
        moved = moved + pltpu.roll(moved, 4, 0)
        weight = total4(jnp.where(fourth, moved, 0.0))
        pair = (x * ROOT * weight - moved) * (PAIR_EPS / ROOT)
        return jnp.where(fourth, 0.0, pair)


def decode_kernel(slabs, blocks, slots, *refs):
    fixed_refs = refs[:slabs]
    counts, owners, others = refs[slabs:]
    me = lax.axis_index("dom").astype(jnp.int32)
    lines = -(-slots // BLK)
    total = slabs * blocks
    place = lax.broadcasted_iota(jnp.int32, owners.shape, 0) * BLK
    place = place + lax.broadcasted_iota(jnp.int32, owners.shape, 1) - UNROLL
    owner = jnp.full(owners.shape, total, jnp.int32)
    other = jnp.zeros(owners.shape, jnp.int32)
    start = jnp.zeros((1, BLK), jnp.int32)
    for slab in range(slabs):
        first = (3 if slab else 6) * blocks
        live = fixed_refs[slab][first : first + 1, :].astype(jnp.int32)
        for line in range(lines):
            at = first + 1 + line
            own = fixed_refs[slab][at : at + 1, :].astype(jnp.int32)
            q = fixed_refs[slab][at + lines : at + lines + 1, :].astype(jnp.int32)
            shift = jnp.where(q >= blocks, 1, 0) + jnp.where(q >= 2 * blocks, 1, 0)
            where = slot_of(slab_of(me, slab, slabs) + shift - 1, me, slabs)
            rank = place - start - line * BLK
            inside = (rank >= 0) & (rank < BLK) & (rank < live - line * BLK)
            rank = jnp.clip(rank, 0, BLK - 1)
            own = jnp.broadcast_to(own + slab * blocks, owners.shape)
            q = jnp.broadcast_to(q + (where - shift) * blocks, owners.shape)
            owner = jnp.where(inside, lanes_from(own, rank), owner)
            other = jnp.where(inside, lanes_from(q, rank), other)
        start = start + live
        if slab == 0:
            mine = (live + UNROLL - 1) // UNROLL
    owners[...] = owner
    others[...] = other
    lane = lax.broadcasted_iota(jnp.int32, (1, BLK), 1)
    counts[...] = jnp.where(lane == 0, mine, (start + UNROLL - 1) // UNROLL)


def steps_kernel(slabs, blocks, *refs):
    counts, owners, others, inv = refs[:4]
    state_refs = refs[4 : 4 + slabs]
    fixed_refs = refs[4 + slabs : 4 + 2 * slabs]
    twin_refs = [None, *refs[4 + 2 * slabs : 3 + 3 * slabs]]
    x_out, v_out, f_out = refs[3 + 3 * slabs : 6 + 3 * slabs]
    xs, vs, ms, w0s, w1s, packed, *rest = refs[6 + 3 * slabs :]
    odd = lax.rem(lax.axis_index("wrow"), 2) == 1
    acc = rest[0]
    total = slabs * blocks
    row, fourth = sub_row(), is_fourth()
    aux = state_refs[0][7 * blocks : 7 * blocks + 1, :]
    centre = [aux[:, k : k + 1] for k in range(2)]
    stiff = [aux[:, k : k + 1] for k in range(2, 4)]
    zero = jnp.zeros((8, BLK), jnp.float32)

    none = jnp.zeros((1, BLK), jnp.float32)

    def strided(ref, t, count):
        return ref[pl.ds(t, count, stride=blocks), :]

    work = Pairs(total, owners, others, *rest)

    sums = (zero, zero)
    for slab in range(slabs):

        def load(group, carry, slab=slab):
            done = []
            for u in range(PASS):
                t = group * PASS + u
                state = jnp.concatenate([strided(state_refs[slab], t, 7), none], 0)
                m = jnp.broadcast_to(state[3:4], (8, BLK))
                state = jnp.where(fourth, 0.0, state)
                turned = pltpu.roll(state, 4, 0)
                x = jnp.where(row < 4, state, turned)
                v = jnp.where(row < 4, turned, state)
                if slab:
                    mine = strided(fixed_refs[slab], t, 3)
                    twin = strided(twin_refs[slab], t, 3)
                else:
                    w = strided(fixed_refs[slab], t, 6)
                    mine, twin = w[:3], w[3:]
                w = jnp.concatenate([mine, none, twin, none], 0)
                turned = pltpu.roll(w, 4, 0)
                w0 = jnp.where(row < 4, w, turned)
                w1 = jnp.where(row < 4, turned, w)
                if slab:
                    w0, w1 = jnp.where(odd, w1, w0), jnp.where(odd, w0, w1)
                carry = carry[0] + w0 * x, carry[1] + w1 * x
                done.append((slab * blocks + t, x, v, m, w0, w1))
            for block, x, v, m, w0, w1 in done:
                xs[block] = x
                vs[block] = v
                ms[block] = m
                w0s[block] = w0
                w1s[block] = w1
            work.tables([(block, x) for block, x, *_ in done])
            return carry

        sums = lax.fori_loop(0, blocks // PASS, load, sums)

    def pulls(pair):
        return [stiff[k] * (0.5 * whole(pair[k]) - centre[k]) for k in range(2)]

    def step(number, sums):
        work.run(counts[0, 1])
        pull = pulls(sums)
        kick = jnp.where(number == 0, jnp.float32(0.5 * DT), jnp.float32(DT))

        def some(group, carry):
            moved = []
            for u in range(WIDE):
                block = group * WIDE + u
                x = xs[block]
                force = work.force(acc[block], x) - (pull[0] * w0s[block] + pull[1] * w1s[block])
                v = vs[block] + kick * ms[block] * force
                x = x + DT * v
                moved.append((block, x, v))
                carry = carry[0] + w0s[block] * x, carry[1] + w1s[block] * x
            for block, x, v in moved:
                xs[block] = x
                vs[block] = v
            work.tables([(block, x) for block, x, _ in moved])
            return carry

        return lax.fori_loop(0, total // WIDE, some, (zero, zero))

    sums = lax.fori_loop(0, STEPS, step, sums)
    work.run(counts[0, 0])
    pull = pulls(sums)

    for block in range(blocks):
        x = xs[block]
        force = work.force(acc[block], x) - (pull[0] * w0s[block] + pull[1] * w1s[block])
        v = vs[block] + (0.5 * DT) * ms[block] * force
        packed[block, 0:8] = jnp.where(row < 4, x, v)
        packed[block, 8:16] = force
    rows = [
        [packed[b, k : k + 1, :] for k in (0, 1, 2, 4, 5, 6, 8, 9, 10)] for b in range(blocks)
    ]
    found = reordered(inv[:blocks, :], inv[blocks:, :], rows)
    for k, value in enumerate(found):
        out = (x_out, v_out, f_out)[k // 3]
        k = k % 3
        out[k * blocks : (k + 1) * blocks, :] = value


def swapped(value, axis, accept):
    pairs = [(i, i ^ 1) for i in range(lax.axis_size(axis))]
    return jnp.where(accept == 1, lax.ppermute(value, axis, pairs), value)


def round_dom(value):
    count = lax.axis_size("dom")
    return [value] + [
        lax.ppermute(value, "dom", [(slab_of(i, s, count), i) for i in range(count)])
        for s in range(1, count)
    ]


def per_device(
    positions,
    velocities,
    inv_mass,
    cv_weight,
    stiffness,
    centers,
    block_order,
    pair_count,
    pair_own,
    pair_other,
    accept_row,
    accept_col,
):
    size = block_order.shape[0]
    blocks = size // BLK
    slots = pair_own.shape[1]
    slabs = lax.axis_size("dom")
    total = slabs * blocks
    vmem = pl.BlockSpec(memory_space=pltpu.VMEM)
    smem = pl.BlockSpec(memory_space=pltpu.SMEM)
    floats = jnp.float32
    tail = -(-(1 + 2 * -(-slots // BLK)) // 8) * 8

    def payload(count):
        return jax.ShapeDtypeStruct((count, BLK), floats)

    def lines(value):
        return value.reshape(-1, BLK)

    def small(flops):
        return dict(
            compiler_params=pltpu.CompilerParams(vmem_limit_bytes=SMALL_VMEM),
            cost_estimate=pl.CostEstimate(
                flops=flops, bytes_accessed=1 << 17, transcendentals=0
            ),
        )

    order = lines(block_order)
    state = pl.pallas_call(
        functools.partial(state_kernel, blocks),
        out_shape=payload(7 * blocks + 8),
        in_specs=[smem] * 2 + [vmem] * 4,
        out_specs=vmem,
    )(centers[0], stiffness, lines(positions), lines(velocities), lines(inv_mass), order)
    weights = cv_weight.reshape(2, 3, blocks, BLK).transpose(1, 2, 0, 3).reshape(-1, BLK)
    fixed, half = pl.pallas_call(
        functools.partial(weight_kernel, blocks, slots),
        out_shape=[payload(6 * blocks + tail), payload(3 * blocks + tail)],
        in_specs=[smem] + [vmem] * 4,
        out_specs=[vmem] * 2,
        **small(1 << 24),
    )(pair_count, weights, order, pair_own, pair_other)
    inverse = pl.pallas_call(
        functools.partial(inverse_kernel, blocks),
        out_shape=jax.ShapeDtypeStruct((2 * blocks, BLK), jnp.int32),
        in_specs=[vmem],
        out_specs=vmem,
        **small(1 << 24),
    )(order)

    state = swapped(state, "wrow", accept_row[0, 0])
    state = swapped(state, "wcol", accept_col[0, 0])
    fixeds = [fixed] + round_dom(half)[1:]
    states = round_dom(state)
    flips = [(i, i ^ 1) for i in range(lax.axis_size("wrow"))]
    twins = [lax.ppermute(value, "wrow", flips) for value in fixeds[1:]]

    room = -(-(slabs * slots + 4 * UNROLL) // (8 * BLK)) * 8
    tables = [(1, BLK)] + [(room, BLK)] * 2
    listed = pl.pallas_call(
        functools.partial(decode_kernel, slabs, blocks, slots),
        out_shape=[jax.ShapeDtypeStruct(shape, jnp.int32) for shape in tables],
        in_specs=[vmem] * slabs,
        out_specs=[vmem] * 3,
        **small(1 << 24),
    )(*fixeds)

    part = pltpu.VMEM((total, 8, BLK), floats)
    outs = pl.pallas_call(
        functools.partial(steps_kernel, slabs, blocks),
        out_shape=[jax.ShapeDtypeStruct((3 * blocks, BLK), floats)] * 3,
        in_specs=[smem] * 3 + [vmem] * (3 * slabs),
        out_specs=[vmem] * 3,
        scratch_shapes=[part] * 5
        + [
            pltpu.VMEM((blocks, 16, BLK), floats),
            pltpu.VMEM((total + 1, 16, BLK), floats),
            pltpu.VMEM((total + 1, 32, BLK), jnp.bfloat16),
            pltpu.VMEM((total, BLK, 32), jnp.bfloat16),
            pltpu.VMEM((total, 16, 2 * BLK), jnp.bfloat16),
            pltpu.VMEM((UNROLL, BLK, BLK), floats),
            pltpu.VMEM((UNROLL, 16, BLK), floats),
        ],
        compiler_params=pltpu.CompilerParams(vmem_limit_bytes=MAIN_VMEM),
    )(*listed, inverse, *states, *fixeds, *twins)
    return tuple(out.reshape(positions.shape) for out in outs)


def solution(mesh):
    placed = (
        P("wrow", "wcol", None, "dom"),
        P("wrow", "wcol", None, "dom"),
        P("dom"),
        P(None, None, "dom"),
        P(),
        P("wrow", "wcol", None),
        P("dom"),
        P("dom"),
        P("dom", None),
        P("dom", None),
        P("wrow", "wcol"),
        P("wrow", "wcol"),
    )
    return jax.shard_map(
        per_device,
        mesh=mesh,
        in_specs=placed,
        out_specs=(P("wrow", "wcol", None, "dom"),) * 3,
        check_vma=False,
    )
```
